512 devices in a mesh: win: 2 (over y), dx: 32 (over z), dy: 4 (over x), dz: 2 (over core).
Axes of the slice: x: 4, y: 2, z: 32, core: 2. Of those that a mesh axis runs over, the one named last changes fastest.
The devices are a block of a 4x8x32 slice.
Arguments:
- fraction: float32 [3, 64, 4, 2, 768], P(None, ('win', 'dx'), 'dy', 'dz'), parts along dimension 1, may hold values from 0 to 1
- atom_type: int32 [64, 4, 2, 768], P(('win', 'dx'), 'dy', 'dz'), parts along dimension 0, may hold values from 0 to 31
- perturbed: int32 [64, 4, 2, 768], P(('win', 'dx'), 'dy', 'dz'), parts along dimension 0, may hold values from 0 to 1
- leaving: int32 [64, 4, 2, 2, 16], P(('win', 'dx'), 'dy', 'dz'), parts along dimension 0, may hold values from 0 to 767, as said below
- neighbours: int32 [64, 4, 2, 6, 16], P(('win', 'dx'), 'dy', 'dz'), parts along dimension 0, may hold values from 0 to 161, as said below
- counts: int32 [64, 4, 2, 6], P(('win', 'dx'), 'dy', 'dz'), parts along dimension 0, may hold values from 1 to 16, as said below
- sigma_table: float32 [32], replicated, may hold values from 0.8 to 1.2
- depth_table: float32 [32], replicated, may hold values from 0.002 to 0.03
- charge_table: float32 [32], replicated, may hold values from -1 to 1
- domain_edge: float32 [3], replicated, may hold values from 1 to 1.12
- coupling: float32 [2], P('win'), parts along dimension 0, may hold values from 0.1 to 0.9
Outputs:
- forces: float32 [3, 64, 4, 2, 768], P(None, ('win', 'dx'), 'dy', 'dz'), parts along dimension 1
- energy: float32 [2], P('win'), parts along dimension 0
- dhdl: float32 [2], P('win'), parts along dimension 0
The draws below stay inside these ranges and needn't reach their ends.
There are 2 independent parts, one for each index of `win`. The reference program is written for one: setup_inputs(seed, part) draws one part's arguments, and reference() takes and returns one part's arrays. A program takes and returns all parts, laid end to end along the dimension named above; an argument that names none is the same for every part. Nothing has to cross between parts.
Inputs may be any that keep to these rules, and one draw needn't show every extreme that they name: `leaving`: each domain lists 2 * 16 distinct slots: the first 16 leave toward the next domain, the last 16 toward the previous one. `neighbours`: each list holds 16 distinct ghost block numbers; entries at or past the block's count are valid numbers and are not used. `counts`: some block lists exactly 16 blocks in every draw.
All inputs are finite; a program needn't handle non-finite values.
Results may differ from the reference program's by a relative error of at most 0.0003.
Values sent between devices are 32-bit elements; how exact they have to be, the bound alone decides.
A program may use at most 64 MiB of HBM per device.

```python
import math
import jax
import jax.numpy as jnp
from jax import lax

ATOMS_DEV = 768
NB = 16
MIG = 16
NTYPES = 32
NATOMS = 196608
N_DX = 32
N_DY = 4
N_DZ = 2


def draw_perturbed(key, part):
    shape = (N_DX, N_DY, N_DZ, ATOMS_DEV)
    position_x = jnp.arange(N_DX, dtype=jnp.int32)[:, None, None, None]
    threshold = 10 + 20 * position_x // max(N_DX - 1, 1)
    values = jax.random.randint(key, shape, 0, 100, dtype=jnp.int32)
    return (values < threshold).astype(jnp.int32)


def draw_leaving(key, part):
    shape = (N_DX, N_DY, N_DZ, ATOMS_DEV)
    scores = jax.random.randint(key, shape, 0, 2 ** 16, dtype=jnp.int32) * ATOMS_DEV + jnp.arange(ATOMS_DEV, dtype=jnp.int32)
    order = jnp.argsort(scores, axis=-1, stable=True).astype(jnp.int32)
    return order[..., :2 * MIG].reshape(N_DX, N_DY, N_DZ, 2, MIG)


def draw_neighbours(key, part):
    ghost_blocks = 27 * (ATOMS_DEV // 128)
    shape = (N_DX, N_DY, N_DZ, ATOMS_DEV // 128, ghost_blocks)
    scores = jax.random.randint(key, shape, 0, 2 ** 16, dtype=jnp.int32) * ghost_blocks + jnp.arange(ghost_blocks, dtype=jnp.int32)
    order = jnp.argsort(scores, axis=-1, stable=True).astype(jnp.int32)
    return order[..., :NB]


def draw_counts(key, part):
    shape = (N_DX, N_DY, N_DZ, ATOMS_DEV // 128)
    values = jax.random.randint(key, shape, 1, NB + 1, dtype=jnp.int32)
    return values.at[0, 0, 0, 0].set(NB)


def touch_ends(array, key, smallest, top_value):
    longest = array.shape.index(max(array.shape))
    spots = []
    for shift in (0, 1):
        where = [jax.random.randint(jax.random.fold_in(key, axis), (), 0, length) for axis, length in enumerate(array.shape)]
        where[longest] = (where[longest] + shift) % array.shape[longest]
        spots.append(tuple(where))
    return array.at[spots[0]].set(smallest).at[spots[1]].set(top_value)


def levels(own_key, extent, cuts, least, high):
    factor_of, own = 1.0, jax.random.fold_in(own_key, 6)
    for dim, parts in cuts:
        steps = jnp.exp(jax.random.uniform(jax.random.fold_in(own, dim), (parts,), jnp.float32, least / len(cuts), high / len(cuts)))
        factor_of = factor_of * jnp.repeat(steps, extent[dim] // parts).reshape([-1 if axis == dim else 1 for axis in range(len(extent))])
    return factor_of


def setup_inputs(seed: int = 0, part: int = 0) -> dict:
    seeds = jax.random.split(jax.random.key(seed), 12)
    part_splits = jax.random.split(jax.random.fold_in(seeds[11], part), 12)
    fraction = jnp.clip(1.0 * jax.random.uniform(part_splits[0], (3, N_DX, N_DY, N_DZ, ATOMS_DEV), jnp.float32) ** levels(part_splits[0], (3, N_DX, N_DY, N_DZ, ATOMS_DEV), ((1, 32), (2, 4), (3, 2)), -0.2, 0.2), 0.0, 1.0)
    atom_type = touch_ends(jax.random.randint(part_splits[1], (N_DX, N_DY, N_DZ, ATOMS_DEV), 0, NTYPES), jax.random.fold_in(part_splits[1], 1), 0, NTYPES - 1).astype(jnp.int32)
    perturbed = draw_perturbed(jax.random.fold_in(jax.random.fold_in(seeds[11], part), 71), part)
    leaving = draw_leaving(jax.random.fold_in(jax.random.fold_in(seeds[11], part), 71), part)
    neighbours = draw_neighbours(jax.random.fold_in(jax.random.fold_in(seeds[11], part), 71), part)
    counts = draw_counts(jax.random.fold_in(jax.random.fold_in(seeds[11], part), 71), part)
    sigma_table = jnp.clip(jnp.exp(jax.random.uniform(seeds[6], (NTYPES,), jnp.float32, math.log(0.8), math.log(1.2))), 0.8, 1.2)
    depth_table = jnp.clip(jnp.exp(jax.random.uniform(seeds[7], (NTYPES,), jnp.float32, math.log(0.002), math.log(0.03))), 0.002, 0.03)
    charge_table = jnp.clip(jax.random.uniform(seeds[8], (NTYPES,), jnp.float32, -1.0, 1.0), -1.0, 1.0)
    domain_edge = jnp.clip(jax.random.uniform(seeds[9], (3,), jnp.float32, 1.0, 1.12), 1.0, 1.12)
    coupling = jnp.clip(jax.random.uniform(part_splits[10], (1,), jnp.float32, 0.1, 0.9), 0.1, 0.9)
    return {"fraction": fraction, "atom_type": atom_type, "perturbed": perturbed, "leaving": leaving, "neighbours": neighbours, "counts": counts, "sigma_table": sigma_table, "depth_table": depth_table, "charge_table": charge_table, "domain_edge": domain_edge, "coupling": coupling}


soft_base = 0.3
soft_alpha = 0.5
charge_base = 0.3
charge_alpha = 0.5
coulomb = 0.1

def lookup(table_row, type_ids):
    onehot = type_ids[None, :] == jnp.arange(table_row.shape[0], dtype=jnp.int32)[:, None]
    return lax.optimization_barrier(jnp.sum(jnp.where(onehot, table_row[:, None], jnp.float32(0.0)), axis=0))

def pair_block(own_block, other_blocks, live_pairs, coupling_value):
    separation = own_block[0:3][None, :, :, None] - other_blocks[:, 0:3][:, :, None, :]
    radius_sq = lax.optimization_barrier(jnp.sum(separation * separation, axis=1))
    sigma_pair = 0.5 * (own_block[3][None, :, None] + other_blocks[:, 3][:, None, :])
    depth_pair = jnp.sqrt(own_block[4][None, :, None] * other_blocks[:, 4][:, None, :])
    charges = own_block[5][None, :, None] * other_blocks[:, 5][:, None, :]
    flagged = jnp.maximum(own_block[6][None, :, None], other_blocks[:, 6][:, None, :])
    scaled = coupling_value * flagged
    sigma_two = sigma_pair * sigma_pair
    sigma_six = sigma_two * sigma_two * sigma_two
    soft_six = sigma_six * (soft_base + soft_alpha * scaled) + radius_sq * radius_sq * radius_sq
    soft_two = charge_base + charge_alpha * scaled + radius_sq
    inverse_six = 1.0 / soft_six
    energy_lj = 4.0 * depth_pair * (sigma_six * sigma_six * inverse_six * inverse_six - sigma_six * inverse_six)
    grad_six = 4.0 * depth_pair * (sigma_six * inverse_six * inverse_six - 2.0 * sigma_six * sigma_six * inverse_six * inverse_six * inverse_six)
    energy_coul = coulomb * charges * lax.rsqrt(soft_two)
    grad_two = -0.5 * energy_coul / soft_two
    weight = 1.0 - scaled
    total_pair = energy_lj + energy_coul
    pair_energy = jnp.sum(weight * total_pair * live_pairs)
    pair_dhdl = jnp.sum(flagged * (-total_pair + weight * (grad_six * sigma_six * soft_alpha + grad_two * charge_alpha)) * live_pairs)
    force_scale = -weight * (6.0 * radius_sq * radius_sq * grad_six + 2.0 * grad_two) * live_pairs
    forces = lax.optimization_barrier(jnp.sum(force_scale[:, None] * separation, axis=(0, 3)))
    return (forces, pair_energy, pair_dhdl)

def block_terms(ghost_rows, listed_blocks, list_count, block_id, block_total, coupling_value):
    centre = 13 * block_total + block_id
    own_block = lax.dynamic_index_in_dim(ghost_rows, centre, 0, keepdims=False)
    other_blocks = jnp.take(ghost_rows, listed_blocks, axis=0)
    valid_slot = (jnp.arange(listed_blocks.shape[0], dtype=jnp.int32) < list_count).astype(jnp.float32)
    is_self = (listed_blocks == centre).astype(jnp.float32)[:, None, None] * jnp.eye(128, dtype=jnp.float32)[None]
    live_pairs = valid_slot[:, None, None] * (1.0 - is_self)
    return pair_block(own_block, other_blocks, live_pairs, coupling_value)

def reference(fraction, atom_type, perturbed, leaving, neighbours, counts, sigma_table, depth_table, charge_table, domain_edge, coupling):
    domains = N_DX * N_DY * N_DZ
    block_total = ATOMS_DEV // 128
    spacing = float(ATOMS_DEV) ** (1.0 / 3.0)
    type_ids = atom_type.reshape(-1)
    payload = jnp.concatenate([fraction.reshape(3, domains, ATOMS_DEV), lookup(sigma_table, type_ids).reshape(1, domains, ATOMS_DEV), lookup(depth_table, type_ids).reshape(1, domains, ATOMS_DEV), lookup(charge_table, type_ids).reshape(1, domains, ATOMS_DEV), perturbed.reshape(1, domains, ATOMS_DEV).astype(jnp.float32)], axis=0)
    leave_slots = leaving.reshape(domains, 2, MIG)
    upward = jnp.take_along_axis(payload, leave_slots[None, :, 0, :], axis=2)
    downward = jnp.take_along_axis(payload, leave_slots[None, :, 1, :], axis=2)
    shift_x = jnp.zeros((7, 1, 1), jnp.float32).at[0].set(1.0)
    from_below = jnp.roll(upward.reshape(7, N_DX, N_DY * N_DZ, MIG), 1, axis=1).reshape(7, domains, MIG) - shift_x
    from_above = jnp.roll(downward.reshape(7, N_DX, N_DY * N_DZ, MIG), -1, axis=1).reshape(7, domains, MIG) + shift_x

    def place(block_rows, down_slots, up_slots, lower_rows, upper_rows):
        return block_rows.at[:, down_slots].set(lower_rows).at[:, up_slots].set(upper_rows)
    moved = jax.vmap(place, in_axes=(1, 0, 0, 1, 1), out_axes=1)(payload, leave_slots[:, 1], leave_slots[:, 0], from_below, from_above)
    moved_grid = moved.reshape(7, N_DX, N_DY, N_DZ, ATOMS_DEV)
    list_flat = neighbours.reshape(domains, block_total, NB)
    count_flat = counts.reshape(domains, block_total)
    coupling_value = coupling[0]

    def one_domain(flat_id):
        index_x = flat_id // (N_DY * N_DZ)
        index_y = flat_id // N_DZ % N_DY
        index_z = flat_id % N_DZ
        pieces = []
        for step_x in range(3):
            for step_y in range(3):
                for step_z in range(3):
                    neighbour_rows = moved_grid[:, (index_x + step_x - 1) % N_DX, (index_y + step_y - 1) % N_DY, (index_z + step_z - 1) % N_DZ]
                    position = jnp.stack([(neighbour_rows[0] + jnp.float32(step_x - 1)) * domain_edge[0] * spacing, (neighbour_rows[1] + jnp.float32(step_y - 1)) * domain_edge[1] * spacing, (neighbour_rows[2] + jnp.float32(step_z - 1)) * domain_edge[2] * spacing], axis=0)
                    pieces.append(jnp.concatenate([position, neighbour_rows[3:]], axis=0))
        ghost_rows = jnp.stack(pieces, 0).reshape(27, 7, block_total, 128).transpose(0, 2, 1, 3).reshape(27 * block_total, 7, 128)
        listed = list_flat[flat_id]
        listed_count = count_flat[flat_id]

        def one_block(block_id):
            return block_terms(ghost_rows, listed[block_id], listed_count[block_id], block_id, block_total, coupling_value)
        forces, energies, dhdls = lax.map(one_block, jnp.arange(block_total, dtype=jnp.int32))
        return (forces.transpose(1, 0, 2).reshape(3, ATOMS_DEV), jnp.sum(energies), jnp.sum(dhdls))
    forces, energies, dhdls = lax.map(one_domain, jnp.arange(domains, dtype=jnp.int32))
    forces = forces.transpose(1, 0, 2).reshape(3, N_DX, N_DY, N_DZ, ATOMS_DEV)
    energy = (0.5 * jnp.sum(energies) / jnp.float32(NATOMS)).reshape(1)
    dhdl = (0.5 * jnp.sum(dhdls) / jnp.float32(NATOMS)).reshape(1)
    return (forces, energy, dhdl)
```

```python
import math

import jax
import jax.numpy as jnp
from jax import lax
from jax.experimental import pallas as pl
from jax.experimental.pallas import tpu as pltpu
from jax.sharding import PartitionSpec as P

F32 = jnp.float32
BF16 = jnp.bfloat16
MESH = pl.DeviceIdType.MESH
HIGHEST = lax.Precision.HIGHEST

SIGMA_SCALE = 0.5 * 4.0 ** (-1.0 / 6.0)
CHARGE_SCALE = math.sqrt(0.1 / math.sqrt(2.0))
PLANE = [(a, b) for a in (-1, 0, 1) for b in (-1, 0, 1)]
CHUNK = 16


def split3(x):
    high = x.astype(BF16)
    rest = x - high.astype(F32)
    mid = rest.astype(BF16)
    low = (rest - mid.astype(F32)).astype(BF16)
    return high, mid, low


def join3(x):
    return x[0:8] + (x[8:16] + x[16:24])


def pair(own, other):
    dx, dy, dz = own[0] - other[0], own[1] - other[1], own[2] - other[2]
    r2 = dx * dx + dy * dy + dz * dz
    c = jnp.maximum(own[6], other[6])
    h = own[3] + other[3]
    h2 = h * h
    s = h2 * h2 * h2
    r4 = r2 * r2
    inverse = 1.0 / (s * c + r4 * r2)
    u = s * inverse
    root = lax.rsqrt(c + r2)
    t = (own[4] * other[4]) * u
    ty = t * (u - 1.0)
    coul = (own[5] * other[5]) * root
    return (dx, dy, dz), c, r4, inverse, u, root, t, ty, coul


def kernel(
    sizes,
    frac_hbm,
    type_hbm,
    pert_hbm,
    leaving,
    neighbours,
    counts,
    sigma_table,
    depth_table,
    charge_table,
    edge,
    coupling,
    forces_out,
    energy_out,
    dhdl_out,
    pay,
    kinds,
    perts,
    table,
    mig_out,
    mig_in,
    mine,
    theirs,
    ghost,
    own,
    force_acc,
    plane_sums,
    line_sums,
    in_sem,
    mig_send,
    mig_recv,
    halo_send,
    halo_recv,
    over_send,
    over_recv,
    plane_send,
    plane_recv,
    line_send,
    line_recv,
    token,
):
    n_dx, n_dy, n_dz, blocks, listed = sizes
    me_x, me_y, me_z = lax.axis_index("dx"), lax.axis_index("dy"), lax.axis_index("dz")

    def along(a, b, c=0):
        return {
            "dx": lax.rem(me_x + a % n_dx, n_dx),
            "dy": lax.rem(me_y + b % n_dy, n_dy),
            "dz": lax.rem(me_z + c, n_dz),
        }

    def signal(semaphore, device):
        pl.semaphore_signal(semaphore, inc=1, device_id=device, device_id_type=MESH)

    peers = [(b, c) for b in range(n_dy) for c in range(n_dz) if (b, c) != (0, 0)]
    near = [(a, b, 0) for a, b in PLANE if a != 0]
    near += [(0, b, c) for b, c in peers]
    barrier = pltpu.get_barrier_semaphore()
    for device in near:
        signal(barrier, along(*device))

    copies = []
    for q in range(blocks):
        lanes = pl.ds(q * 128, 128)
        for k in range(3):
            copies.append((frac_hbm.at[k, 0, 0, 0, lanes], pay.at[q, k]))
        copies.append((type_hbm.at[0, 0, 0, lanes], kinds.at[q]))
        copies.append((pert_hbm.at[0, 0, 0, lanes], perts.at[q]))
    copies = [
        pltpu.make_async_copy(src, dst, in_sem.at[i]) for i, (src, dst) in enumerate(copies)
    ]
    for copy in copies:
        copy.start()

    lam = coupling[0]
    sub = lax.broadcasted_iota(jnp.int32, (32, 128), 0)
    lane8 = lax.broadcasted_iota(jnp.int32, (8, 128), 1)
    gather_slots = jnp.zeros((8, 128), jnp.int32)
    scatter_slots = jnp.zeros((32, 128), jnp.int32)
    for m in range(32):
        down = leaving[0, 0, 0, 1 - m // 16, m % 16]
        home = leaving[0, 0, 0, m // 16, m % 16]
        gather_slots = jnp.where(lane8 == m, down, gather_slots)
        scatter_slots = jnp.where(sub == m, home, scatter_slots)
    gather_slots = jnp.where(lane8 < 32, gather_slots, -1)

    for copy in copies:
        copy.wait()
    kind = kinds[0:blocks, :]
    sigma = jnp.zeros((blocks, 128), F32)
    depth = jnp.zeros((blocks, 128), F32)
    charge = jnp.zeros((blocks, 128), F32)
    for k in range(sigma_table.shape[0]):
        hit = kind == k
        sigma = jnp.where(hit, sigma_table[k], sigma)
        depth = jnp.where(hit, depth_table[k], depth)
        charge = jnp.where(hit, charge_table[k], charge)
    flag = perts[0:blocks, :].astype(F32)
    table[0] = sigma * SIGMA_SCALE
    table[1] = jnp.sqrt(depth)
    table[2] = charge * CHARGE_SCALE
    table[3] = 0.15 + (0.25 * lam) * flag
    table[4] = flag
    for q in range(blocks):
        for k in range(5):
            pay[q, 3 + k : 4 + k, :] = table[k, q : q + 1, :]

    rows = lax.broadcasted_iota(jnp.int32, (128, 128), 0)
    gathered = jnp.zeros((24, 128), F32)
    for q in range(blocks):
        pick = (gather_slots[0:1] == rows + q * 128).astype(F32).astype(BF16)
        parts = jnp.concatenate(split3(pay[q]), axis=0)
        gathered += jnp.dot(parts, pick, preferred_element_type=F32)
    mig_out[...] = join3(gathered)

    pl.semaphore_wait(barrier, len(near))
    for a in (-1, 1):
        signal(token.at[0], along(a, 0))
    moves = []
    for i, a in enumerate((1, -1)):
        moves.append(
            pltpu.make_async_remote_copy(
                mig_out, mig_in.at[i], mig_send.at[i], mig_recv.at[i], along(a, 0), MESH
            )
        )
    for move in moves:
        move.start()

    spacing = float(blocks * 128) ** (1.0 / 3.0) * math.sqrt(0.5)
    row8 = lax.broadcasted_iota(jnp.int32, (8, 128), 0)
    scale = jnp.ones((8, 128), F32)
    for k in range(3):
        scale = jnp.where(row8 == k, edge[k] * spacing, scale)

    def placed(tile, a, b, c):
        step = jnp.zeros((8, 128), F32)
        for k, value in enumerate((a, b, c)):
            if value:
                step = jnp.where(row8 == k, float(value), step)
        return (tile + step) * scale

    for move in moves:
        move.wait()
    tile = jnp.where(lane8 < 16, mig_in[1], mig_in[0])
    step_x = jnp.where(row8 == 0, jnp.where(lane8 < 16, 1.0, -1.0), 0.0)
    parts = jnp.concatenate((*split3(tile + step_x), jnp.ones((8, 128), BF16)), axis=0)
    lane32 = lax.broadcasted_iota(jnp.int32, (32, 128), 1)
    for q in range(blocks):
        spread = (scatter_slots == lane32 + q * 128).astype(F32).astype(BF16)
        landed = jnp.dot(parts[:, 0:32], spread, preferred_element_type=F32)
        mine[4, q] = jnp.where(landed[24:32] > 0.5, join3(landed), pay[q])

    sends = []
    for i, (a, b) in enumerate(PLANE):
        if (a, b) != (0, 0):
            sends.append(
                pltpu.make_async_remote_copy(
                    mine.at[4], mine.at[i], halo_send.at[i], halo_recv.at[i], along(-a, -b), MESH
                )
            )
    for send in sends:
        send.start()

    def over(i):
        return pltpu.make_async_remote_copy(
            mine.at[i], theirs.at[i], over_send.at[i], over_recv.at[i], along(0, 0, 1), MESH
        )

    overs = {4: over(4)}
    overs[4].start()
    pl.semaphore_wait(token.at[0], 2)
    for a in (-2, 2):
        signal(token.at[1], along(a, 0))

    center = 13 * blocks
    for q in range(blocks):
        ghost[center + q] = placed(mine[4, q], 0, 0, 0)
    ghost[27 * blocks] = jnp.where(row8 == 3, 1.0, jnp.where(row8 == 6, 0.15, 0.0))
    for q in range(blocks):
        columns = ghost[center + q].T
        for k in range(8):
            own[k, q * 128 : q * 128 + 128, :] = jnp.broadcast_to(
                columns[:, k : k + 1], (128, 128)
            )

    pl.semaphore_wait(token.at[1], 2)
    for a in (-4, 4):
        signal(token.at[2], along(a, 0))
    order = [i for i, (a, b) in enumerate(PLANE) if abs(a) + abs(b) == 1]
    order += [i for i, (a, b) in enumerate(PLANE) if abs(a) + abs(b) == 2]
    by_slot = dict(zip([i for i in range(9) if i != 4], sends))
    for i in order:
        by_slot[i].wait_recv()
        overs[i] = over(i)
        overs[i].start()
        a, b = PLANE[i]
        for q in range(blocks):
            ghost[(3 * i + 1) * blocks + q] = placed(mine[i, q], a, b, 0)
    pl.semaphore_wait(token.at[2], 2)
    for a in (-8, 8):
        signal(token.at[3], along(a, 0))
    for i in [4] + order:
        overs[i].wait_recv()
        a, b = PLANE[i]
        for q in range(blocks):
            for c in (-1, 1):
                ghost[(3 * i + 1 + c) * blocks + q] = placed(theirs[i, q], a, b, c)
    for i in range(9):
        if i != 4:
            by_slot[i].wait_send()
        overs[i].wait_send()

    steps = blocks * 128 // CHUNK
    per_block = 128 // CHUNK
    halves = CHUNK // 8

    def block_number(q, e):
        used = e < counts[0, 0, 0, q]
        return jnp.where(used, neighbours[0, 0, 0, q, e], 27 * blocks)

    def own_rows(k):
        return [
            [own[r, pl.ds(k * CHUNK + 8 * half, 8), :] for r in range(8)] for half in range(halves)
        ]

    def other_rows(q, e):
        number = block_number(q, e)
        return [ghost[number, r : r + 1, :] for r in range(8)]

    def energy_step(k, sums):
        q = k // per_block
        atoms = own_rows(k)
        v_sum, pv_sum, pg_sum = sums
        for e in range(listed):
            other = other_rows(q, e)
            for atom in atoms:
                _, _, _, _, u, root, t, ty, coul = pair(atom, other)
                p = jnp.maximum(atom[7], other[7])
                v = (ty - t) + coul
                g = u * ty + 0.25 * (coul * (root * root))
                v_sum, pv_sum, pg_sum = v_sum + v, pv_sum + p * v, pg_sum + p * g
        return v_sum, pv_sum, pg_sum

    zero = jnp.zeros((8, 128), F32)
    v_sum, pv_sum, pg_sum = lax.fori_loop(0, steps, energy_step, (zero, zero, zero))
    v_row = jnp.sum(v_sum, axis=0, keepdims=True)
    pv_row = jnp.sum(pv_sum, axis=0, keepdims=True)
    pg_row = jnp.sum(pg_sum, axis=0, keepdims=True)
    for q in range(blocks):
        itself = jnp.float32(0.0)
        for e in range(listed):
            itself += jnp.where(block_number(q, e) == center + q, 1.0, 0.0)
        tile = ghost[center + q]
        atom = [tile[r : r + 1] for r in range(8)]
        _, _, _, _, u, root, t, ty, coul = pair(atom, atom)
        v = (ty - t) + coul
        g = u * ty + 0.25 * (coul * (root * root))
        v_row -= itself * v
        pv_row -= itself * (atom[7] * v)
        pg_row -= itself * (atom[7] * g)
    energy_row = v_row - lam * pv_row
    dhdl_row = -pv_row - (0.5 * (1.0 - lam)) * pg_row
    lane1 = lax.broadcasted_iota(jnp.int32, (1, 128), 1)
    energy_row += pltpu.roll(energy_row, 64, 1)
    dhdl_row += pltpu.roll(dhdl_row, 64, 1)
    part = jnp.where(lane1 < 64, energy_row, dhdl_row)

    my_peer = me_y * n_dz + me_z
    plane_sums[my_peer] = part
    plane_copies = []
    for i, (b, c) in enumerate(peers):
        plane_copies.append(
            pltpu.make_async_remote_copy(
                plane_sums.at[my_peer],
                plane_sums.at[my_peer],
                plane_send.at[i],
                plane_recv.at[i],
                along(0, b, c),
                MESH,
            )
        )
    for copy in plane_copies:
        copy.start()

    def force_step(k, carry):
        q = k // per_block
        atoms = own_rows(k)
        sums = [[jnp.zeros((8, 128), F32)] * 3 for _ in atoms]
        twelve = [atom[4] * 12.0 for atom in atoms]
        atoms = [atom[:4] + [big] + atom[5:] for atom, big in zip(atoms, twelve)]
        for e in range(listed):
            other = other_rows(q, e)
            for half, atom in enumerate(atoms):
                d, c, r4, inverse, _, root, _, ty, coul = pair(atom, other)
                f = (r4 * inverse) * ty + coul * (root * root)
                f *= 1.6 - 4.0 * c
                sums[half] = [total + f * part for total, part in zip(sums[half], d)]
        for half, totals in enumerate(sums):
            for axis, total in enumerate(totals):
                force_acc[axis, pl.ds(k * CHUNK + 8 * half, 8), :] = total
        return carry

    first = steps // 3
    lax.fori_loop(0, first, force_step, 0)
    for copy in plane_copies:
        copy.wait()
    total = plane_sums[0]
    for i in range(1, n_dy * n_dz):
        total = total + plane_sums[i]
    line_sums[me_x] = total
    pl.semaphore_wait(token.at[3], 2)
    line_copies = []
    for d in range(1, n_dx):
        line_copies.append(
            pltpu.make_async_remote_copy(
                line_sums.at[me_x],
                line_sums.at[me_x],
                line_send.at[d],
                line_recv.at[d],
                along(d, 0),
                MESH,
            )
        )
    for copy in line_copies:
        copy.start()

    lax.fori_loop(first, steps, force_step, 0)
    ones = jnp.ones((8, 128), F32)
    for q in range(blocks):
        for axis in range(3):
            sums = lax.dot_general(
                ones,
                force_acc[axis, q * 128 : q * 128 + 128, :],
                (((1,), (1,)), ((), ())),
                precision=HIGHEST,
                preferred_element_type=F32,
            )
            forces_out[axis, 0, 0, :, q * 128 : q * 128 + 128] = sums[0:1] * math.sqrt(0.5)

    for copy in line_copies:
        copy.wait()
    total = line_sums[0]
    for i in range(1, n_dx):
        total = total + line_sums[i]
    norm = 0.5 / (blocks * 128 * n_dx * n_dy * n_dz)
    energy_out[0] = jnp.sum(jnp.where(lane1 < 64, total, 0.0)) * norm
    dhdl_out[0] = jnp.sum(jnp.where(lane1 < 64, 0.0, total)) * norm


def on_device(
    fraction,
    atom_type,
    perturbed,
    leaving,
    neighbours,
    counts,
    sigma_table,
    depth_table,
    charge_table,
    domain_edge,
    coupling,
):
    n_dx, n_dy, n_dz = (lax.axis_size(axis) for axis in ("dx", "dy", "dz"))
    atoms = fraction.shape[-1]
    blocks = atoms // 128
    sizes = (n_dx, n_dy, n_dz, blocks, neighbours.shape[-1])
    hbm = pl.BlockSpec(memory_space=pl.ANY)
    smem = pl.BlockSpec(memory_space=pltpu.SMEM)
    dma, regular = pltpu.SemaphoreType.DMA, pltpu.SemaphoreType.REGULAR
    return pl.pallas_call(
        lambda *refs: kernel(sizes, *refs),
        out_shape=(
            jax.ShapeDtypeStruct(fraction.shape, F32),
            jax.ShapeDtypeStruct((1,), F32),
            jax.ShapeDtypeStruct((1,), F32),
        ),
        in_specs=[hbm] * 3 + [smem] * 8,
        out_specs=(pl.BlockSpec(memory_space=pltpu.VMEM), smem, smem),
        scratch_shapes=[
            pltpu.VMEM((blocks, 8, 128), F32),
            pltpu.VMEM((8, 128), jnp.int32),
            pltpu.VMEM((8, 128), jnp.int32),
            pltpu.VMEM((5, blocks, 128), F32),
            pltpu.VMEM((8, 128), F32),
            pltpu.VMEM((2, 8, 128), F32),
            pltpu.VMEM((9, blocks, 8, 128), F32),
            pltpu.VMEM((9, blocks, 8, 128), F32),
            pltpu.VMEM((27 * blocks + 1, 8, 128), F32),
            pltpu.VMEM((8, atoms, 128), F32),
            pltpu.VMEM((3, atoms, 128), F32),
            pltpu.VMEM((n_dy * n_dz, 1, 128), F32),
            pltpu.VMEM((n_dx, 1, 128), F32),
            dma((5 * blocks,)),
            dma((2,)),
            dma((2,)),
            dma((9,)),
            dma((9,)),
            dma((9,)),
            dma((9,)),
            dma((n_dy * n_dz,)),
            dma((n_dy * n_dz,)),
            dma((n_dx,)),
            dma((n_dx,)),
            regular((4,)),
        ],
        compiler_params=pltpu.CompilerParams(
            collective_id=0, has_side_effects=True, vmem_limit_bytes=48 * 1024 * 1024
        ),
        name="step",
    )(
        fraction,
        atom_type,
        perturbed,
        leaving,
        neighbours,
        counts,
        sigma_table,
        depth_table,
        charge_table,
        domain_edge,
        coupling,
    )


def solution(mesh):
    return jax.shard_map(
        on_device,
        mesh=mesh,
        in_specs=(
            P(None, ("win", "dx"), "dy", "dz", None),
            P(("win", "dx"), "dy", "dz", None),
            P(("win", "dx"), "dy", "dz", None),
            P(("win", "dx"), "dy", "dz", None, None),
            P(("win", "dx"), "dy", "dz", None, None),
            P(("win", "dx"), "dy", "dz", None),
            P(),
            P(),
            P(),
            P(),
            P("win"),
        ),
        out_specs=(P(None, ("win", "dx"), "dy", "dz", None), P("win"), P("win")),
        check_vma=False,
    )
```

```python
import math

import jax
import jax.numpy as jnp
from jax import lax
from jax.experimental import pallas as pl
from jax.experimental.pallas import tpu as pltpu
from jax.sharding import PartitionSpec as P

F32 = jnp.float32
BF16 = jnp.bfloat16
MESH = pl.DeviceIdType.MESH

SIGMA_SCALE = 0.5 * 4.0 ** (-1.0 / 6.0)
CHARGE_SCALE = math.sqrt(0.1 / math.sqrt(2.0))
FORCE_SCALE = 12.0 * math.sqrt(0.5)
CENTRE = 4
LEAVE_CENTRE = 7
CHUNK = 16


def split3(x):
    high = x.astype(BF16)
    rest = x - high.astype(F32)
    mid = rest.astype(BF16)
    low = (rest - mid.astype(F32)).astype(BF16)
    return high, mid, low


def join3(x):
    return x[0:8] + (x[8:16] + x[16:24])


def pair(own, other):
    dx, dy, dz = own[0] - other[0], own[1] - other[1], own[2] - other[2]
    r2 = dx * dx + dy * dy + dz * dz
    c = jnp.maximum(own[6], other[6])
    h = own[3] + other[3]
    h2 = h * h
    s = h2 * h2 * h2
    r4 = r2 * r2
    inverse = 1.0 / (s * c + r4 * r2)
    u = s * inverse
    root = lax.rsqrt(c + r2)
    t = (own[4] * other[4]) * u
    ty = t * (u - 1.0)
    coul = (own[5] * other[5]) * root
    return (dx, dy, dz), c, r4, inverse, u, root, t, ty, coul


def kernel(
    sizes,
    frac_hbm,
    type_hbm,
    pert_hbm,
    leaving_hbm,
    neighbours_hbm,
    counts_hbm,
    sigma_hbm,
    depth_hbm,
    charge_hbm,
    edge_hbm,
    coupling_hbm,
    forces_out,
    energy_out,
    dhdl_out,
    leaving,
    neighbours,
    counts,
    sigma_table,
    depth_table,
    charge_table,
    edge,
    coupling,
    kinds,
    perts,
    table,
    raw,
    leavers,
    theirs,
    ghost,
    own,
    force_acc,
    plane_sums,
    line_sums,
    in_sem,
    leave_send,
    leave_recv,
    halo_send,
    halo_recv,
    over_send,
    over_recv,
    plane_send,
    plane_recv,
    line_send,
    line_recv,
    token,
):
    n_dx, n_dy, n_dz, blocks, listed = sizes
    me_x, me_y, me_z = lax.axis_index("dx"), lax.axis_index("dy"), lax.axis_index("dz")

    def along(a, b, c=0):
        return {
            "dx": lax.rem(me_x + a % n_dx, n_dx),
            "dy": lax.rem(me_y + b % n_dy, n_dy),
            "dz": lax.rem(me_z + c, n_dz),
        }

    def signal(semaphore, device):
        pl.semaphore_signal(semaphore, inc=1, device_id=device, device_id_type=MESH)

    copies = [
        (leaving_hbm, leaving),
        (sigma_hbm, sigma_table),
        (depth_hbm, depth_table),
        (charge_hbm, charge_table),
        (coupling_hbm, coupling),
        (edge_hbm, edge),
        (neighbours_hbm, neighbours),
        (counts_hbm, counts),
    ]
    for q in range(blocks):
        lanes = pl.ds(q * 128, 128)
        for k in range(3):
            copies.append((frac_hbm.at[k, 0, 0, 0, lanes], raw.at[CENTRE, q, k]))
        copies.append((type_hbm.at[0, 0, 0, lanes], kinds.at[q]))
        copies.append((pert_hbm.at[0, 0, 0, lanes], perts.at[q]))
    copies = [
        pltpu.make_async_copy(src, dst, in_sem.at[i]) for i, (src, dst) in enumerate(copies)
    ]
    for copy in copies:
        copy.start()

    peers = [(b, c) for b in range(n_dy) for c in range(n_dz) if (b, c) != (0, 0)]
    near = [(a, b, 0) for a in (1, -1, 2, -2) for b in (0, 1, -1)]
    near += [(0, b, c) for b, c in peers]
    barrier = pltpu.get_barrier_semaphore()
    for device in near:
        signal(barrier, along(*device))

    row8 = lax.broadcasted_iota(jnp.int32, (8, 128), 0)
    lane8 = lax.broadcasted_iota(jnp.int32, (8, 128), 1)
    for copy in copies:
        copy.wait()
    lam = coupling[0]
    leave_slots = jnp.full((8, 128), -1, jnp.int32)
    land_slots = jnp.full((8, 128), -1, jnp.int32)
    for m in range(16):
        up, down = leaving[0, 0, 0, 0, m], leaving[0, 0, 0, 1, m]
        leave_slots = jnp.where(lane8 == m, down, jnp.where(lane8 == m + 16, up, leave_slots))
        land_slots = jnp.where(lane8 == m, up, jnp.where(lane8 == m + 16, down, land_slots))
    kind = kinds[0:blocks, :]
    sigma = jnp.zeros((blocks, 128), F32)
    depth = jnp.zeros((blocks, 128), F32)
    charge = jnp.zeros((blocks, 128), F32)
    for k in range(sigma_table.shape[0]):
        hit = kind == k
        sigma = jnp.where(hit, sigma_table[k], sigma)
        depth = jnp.where(hit, depth_table[k], depth)
        charge = jnp.where(hit, charge_table[k], charge)
    flag = perts[0:blocks, :].astype(F32)
    table[0] = sigma * SIGMA_SCALE
    table[1] = jnp.sqrt(depth)
    table[2] = charge * CHARGE_SCALE
    table[3] = flag
    for q in range(blocks):
        for k in range(5):
            raw[CENTRE, q, 3 + k : 4 + k, :] = table[min(k, 3), q : q + 1, :]

    rows = lax.broadcasted_iota(jnp.int32, (128, 128), 0)
    gathered = jnp.zeros((24, 128), F32)
    for q in range(blocks):
        pick = (leave_slots[0:1] == rows + q * 128).astype(F32).astype(BF16)
        parts = jnp.concatenate(split3(raw[CENTRE, q]), axis=0)
        gathered += jnp.dot(parts, pick, preferred_element_type=F32)
    leavers[LEAVE_CENTRE] = jnp.where(row8 == 7, land_slots.astype(F32), join3(gathered))

    pl.semaphore_wait(barrier, len(near))
    leaves, halos = {}, {}
    for a in (1, -1, 2, -2, 0):
        for b in (0, 1, -1):
            if (a, b) != (0, 0):
                i = 3 * (a + 2) + b + 1
                leaves[a, b] = pltpu.make_async_remote_copy(
                    leavers.at[LEAVE_CENTRE],
                    leavers.at[i],
                    leave_send.at[i],
                    leave_recv.at[i],
                    along(-a, -b),
                    MESH,
                )
                leaves[a, b].start()
    for a, b in ((-1, 0), (1, 0), (0, 1), (0, -1), (1, 1), (-1, 1), (1, -1), (-1, -1)):
        i = 3 * (a + 1) + b + 1
        halos[a, b] = pltpu.make_async_remote_copy(
            raw.at[CENTRE],
            raw.at[i],
            halo_send.at[i],
            halo_recv.at[i],
            along(-a, -b),
            MESH,
        )
        halos[a, b].start()
    for a in (-2, 2):
        signal(token.at[0], along(a, 0))

    spacing = float(blocks * 128) ** (1.0 / 3.0) * math.sqrt(0.5)
    scale = jnp.ones((8, 128), F32)
    for k in range(3):
        scale = jnp.where(row8 == k, edge[k] * spacing, scale)
    scale = jnp.where(row8 == 6, 0.25 * lam, jnp.where(row8 == 7, -lam, scale))
    base = jnp.where(row8 == 6, 0.15, jnp.where(row8 == 7, 1.0, 0.0))
    step_z = jnp.where(row8 == 2, scale, 0.0)
    lane32 = lax.broadcasted_iota(jnp.int32, (32, 128), 1).astype(F32)
    step_x = jnp.where(row8 == 0, jnp.where(lane8 < 16, 1.0, -1.0), 0.0)
    ones8 = jnp.ones((8, 128), BF16)
    seen = set()

    def arrived(a, b):
        if (a, b) != (0, 0) and (a, b) not in seen:
            seen.add((a, b))
            leaves[a, b].wait_recv()
        return leavers.at[3 * (a + 2) + b + 1]

    overs = []

    def settle(a, b):
        i = 3 * (a + 1) + b + 1
        here, above, below = arrived(a, b), arrived(a + 1, b), arrived(a - 1, b)
        if (a, b) != (0, 0):
            halos[a, b].wait_recv()
        slots = jnp.broadcast_to(here[...].T[0:32, 7:8], (32, 128))
        tile = jnp.where(lane8 < 16, above[...], below[...]) + step_x
        tile = jnp.where(row8 == 7, pltpu.roll(tile, 1, 0), tile)
        parts = jnp.concatenate((*split3(tile), ones8), axis=0)
        offset = base
        for k, value in enumerate((a, b)):
            if value:
                offset = jnp.where(row8 == k, scale * float(value), offset)
        for q in range(blocks):
            spread = (slots == lane32 + float(q * 128)).astype(F32).astype(BF16)
            landed = jnp.dot(parts[:, 0:32], spread, preferred_element_type=F32)
            moved = jnp.where(landed[24:32] > 0.5, join3(landed), raw[i, q])
            ghost[(3 * i + 1) * blocks + q] = moved * scale + offset
        over = pltpu.make_async_remote_copy(
            ghost.at[pl.ds((3 * i + 1) * blocks, blocks)],
            theirs.at[i],
            over_send.at[i],
            over_recv.at[i],
            along(0, 0, 1),
            MESH,
        )
        over.start()
        overs.append((i, over))

    ghost[27 * blocks] = jnp.where(
        row8 == 3, 1.0, jnp.where(row8 == 6, 0.15, jnp.where(row8 == 7, 1.0, 0.0))
    )
    settle(0, 0)
    center = 13 * blocks
    for q in range(blocks):
        columns = ghost[center + q].T
        for k in range(8):
            own[k, q * 128 : q * 128 + 128, :] = jnp.broadcast_to(
                columns[:, k : k + 1], (128, 128)
            )

    def block_number(q, e):
        used = e < counts[0, 0, 0, q]
        return jnp.where(used, neighbours[0, 0, q, 0, e], 27 * blocks)

    self_sums = [jnp.zeros((1, 128), F32)] * 3
    for q in range(blocks):
        itself = jnp.float32(0.0)
        for e in range(listed):
            itself += jnp.where(block_number(q, e) == center + q, 1.0, 0.0)
        tile = ghost[center + q]
        atom = [tile[r : r + 1] for r in range(8)]
        _, _, _, _, u, root, t, ty, coul = pair(atom, atom)
        v = (ty - t) + coul
        g = u * ty + 0.25 * (coul * (root * root))
        off = 1.0 - atom[7]
        self_sums = [
            total + itself * term for total, term in zip(self_sums, (v, off * v, off * g))
        ]

    for b in (0, 1, -1):
        settle(-1, b)
    pl.semaphore_wait(token.at[0], 2)
    for a in (-4, 4):
        signal(token.at[1], along(a, 0))
    for a, b in ((0, 1), (0, -1), (1, 0), (1, 1), (1, -1)):
        settle(a, b)
    for i, over in overs:
        over.wait_recv()
        for q in range(blocks):
            for c in (-1, 1):
                ghost[(3 * i + 1 + c) * blocks + q] = theirs[i, q] + (step_z * float(c))
    for copy in (*leaves.values(), *halos.values()):
        copy.wait_send()
    for _, over in overs:
        over.wait_send()

    steps = blocks * 128 // CHUNK
    per_block = 128 // CHUNK
    halves = CHUNK // 8

    def pair_step(k, sums):
        q = k // per_block
        atoms = [
            [own[r, pl.ds(k * CHUNK + 8 * half, 8), :] for r in range(8)] for half in range(halves)
        ]
        v_sum, ov_sum, og_sum = sums
        force = [[jnp.zeros((8, 128), F32)] * 3 for _ in atoms]
        for e in range(listed):
            number = block_number(q, e)
            other = [ghost[number, r : r + 1, :] for r in range(8)]
            for half, atom in enumerate(atoms):
                d, _, r4, inverse, u, root, t, ty, coul = pair(atom, other)
                w = jnp.minimum(atom[7], other[7])
                off = 1.0 - w
                v = (ty - t) + coul
                m = coul * (root * root)
                g = u * ty + 0.25 * m
                v_sum, ov_sum, og_sum = v_sum + v, ov_sum + off * v, og_sum + off * g
                f = ((r4 * inverse) * ty + m * (1.0 / 12.0)) * w
                force[half] = [total + f * part for total, part in zip(force[half], d)]
        for half, totals in enumerate(force):
            for axis, total in enumerate(totals):
                force_acc[axis, pl.ds(k * CHUNK + 8 * half, 8), :] = total
        return v_sum, ov_sum, og_sum

    zero = jnp.zeros((8, 128), F32)
    third = steps // 3
    sums = lax.fori_loop(0, third, pair_step, (zero, zero, zero))
    pl.semaphore_wait(token.at[1], 2)
    for a in (-8, 8):
        signal(token.at[2], along(a, 0))
    sums = lax.fori_loop(third, steps, pair_step, sums)
    v_row, ov_row, og_row = (
        jnp.sum(total, axis=0, keepdims=True) - itself for total, itself in zip(sums, self_sums)
    )
    lane1 = lax.broadcasted_iota(jnp.int32, (1, 128), 1)
    energy_row = v_row - ov_row
    dhdl_row = ov_row + (0.5 * (1.0 - lam)) * og_row
    energy_row += pltpu.roll(energy_row, 64, 1)
    dhdl_row += pltpu.roll(dhdl_row, 64, 1)
    part = jnp.where(lane1 < 64, energy_row, dhdl_row)

    my_peer = me_y * n_dz + me_z
    plane_sums[my_peer] = part
    plane_copies = []
    for i, (b, c) in enumerate(peers):
        plane_copies.append(
            pltpu.make_async_remote_copy(
                plane_sums.at[my_peer],
                plane_sums.at[my_peer],
                plane_send.at[i],
                plane_recv.at[i],
                along(0, b, c),
                MESH,
            )
        )
    for copy in plane_copies:
        copy.start()

    ones = jnp.ones((8, 384), BF16)

    def row_sums(axis):
        for q in range(blocks):
            parts = jnp.concatenate(
                split3(force_acc[axis, q * 128 : q * 128 + 128, :]), axis=1
            )
            total = lax.dot_general(
                ones, parts, (((1,), (1,)), ((), ())), preferred_element_type=F32
            )
            forces_out[axis, 0, 0, :, q * 128 : q * 128 + 128] = total[0:1] * FORCE_SCALE

    row_sums(0)
    row_sums(1)
    for copy in plane_copies:
        copy.wait()
    total = plane_sums[0]
    for i in range(1, n_dy * n_dz):
        total = total + plane_sums[i]
    line_sums[me_x] = total
    pl.semaphore_wait(token.at[2], 2)
    line_copies = []
    for d in sorted(range(1, n_dx), key=lambda d: min(d, n_dx - d)):
        line_copies.append(
            pltpu.make_async_remote_copy(
                line_sums.at[me_x],
                line_sums.at[me_x],
                line_send.at[d],
                line_recv.at[d],
                along(d, 0),
                MESH,
            )
        )
    for copy in line_copies:
        copy.start()
    row_sums(2)
    for copy in line_copies:
        copy.wait()
    total = line_sums[0]
    for i in range(1, n_dx):
        total = total + line_sums[i]
    norm = 0.5 / (blocks * 128 * n_dx * n_dy * n_dz)
    energy_out[0] = jnp.sum(jnp.where(lane1 < 64, total, 0.0)) * norm
    dhdl_out[0] = jnp.sum(jnp.where(lane1 < 64, 0.0, total)) * (-norm / lam)


def on_device(
    fraction,
    atom_type,
    perturbed,
    leaving,
    neighbours,
    counts,
    sigma_table,
    depth_table,
    charge_table,
    domain_edge,
    coupling,
):
    n_dx, n_dy, n_dz = (lax.axis_size(axis) for axis in ("dx", "dy", "dz"))
    atoms = fraction.shape[-1]
    blocks = atoms // 128
    sizes = (n_dx, n_dy, n_dz, blocks, neighbours.shape[-1])
    neighbours = neighbours.transpose(0, 1, 3, 2, 4)
    hbm = pl.BlockSpec(memory_space=pltpu.HBM)
    smem = pl.BlockSpec(memory_space=pltpu.SMEM)
    dma, regular = pltpu.SemaphoreType.DMA, pltpu.SemaphoreType.REGULAR
    scalars = (
        leaving,
        neighbours,
        counts,
        sigma_table,
        depth_table,
        charge_table,
        domain_edge,
        coupling,
    )
    return pl.pallas_call(
        lambda *refs: kernel(sizes, *refs),
        out_shape=(
            jax.ShapeDtypeStruct(fraction.shape, F32),
            jax.ShapeDtypeStruct((1,), F32),
            jax.ShapeDtypeStruct((1,), F32),
        ),
        in_specs=[hbm] * 11,
        out_specs=(pl.BlockSpec(memory_space=pltpu.VMEM), smem, smem),
        scratch_shapes=[
            *[pltpu.SMEM(array.shape, array.dtype) for array in scalars],
            pltpu.VMEM((8, 128), jnp.int32),
            pltpu.VMEM((8, 128), jnp.int32),
            pltpu.VMEM((4, blocks, 128), F32),
            pltpu.VMEM((9, blocks, 8, 128), F32),
            pltpu.VMEM((15, 8, 128), F32),
            pltpu.VMEM((9, blocks, 8, 128), F32),
            pltpu.VMEM((27 * blocks + 1, 8, 128), F32),
            pltpu.VMEM((8, atoms, 128), F32),
            pltpu.VMEM((3, atoms, 128), F32),
            pltpu.VMEM((n_dy * n_dz, 1, 128), F32),
            pltpu.VMEM((n_dx, 1, 128), F32),
            dma((8 + 5 * blocks,)),
            dma((15,)),
            dma((15,)),
            dma((9,)),
            dma((9,)),
            dma((9,)),
            dma((9,)),
            dma((n_dy * n_dz,)),
            dma((n_dy * n_dz,)),
            dma((n_dx,)),
            dma((n_dx,)),
            regular((3,)),
        ],
        compiler_params=pltpu.CompilerParams(
            collective_id=0, has_side_effects=True, vmem_limit_bytes=62 * 1024 * 1024
        ),
        name="step",
    )(
        fraction,
        atom_type,
        perturbed,
        leaving,
        neighbours,
        counts,
        sigma_table,
        depth_table,
        charge_table,
        domain_edge,
        coupling,
    )


def solution(mesh):
    return jax.shard_map(
        on_device,
        mesh=mesh,
        in_specs=(
            P(None, ("win", "dx"), "dy", "dz", None),
            P(("win", "dx"), "dy", "dz", None),
            P(("win", "dx"), "dy", "dz", None),
            P(("win", "dx"), "dy", "dz", None, None),
            P(("win", "dx"), "dy", "dz", None, None),
            P(("win", "dx"), "dy", "dz", None),
            P(),
            P(),
            P(),
            P(),
            P("win"),
        ),
        out_specs=(P(None, ("win", "dx"), "dy", "dz", None), P("win"), P("win")),
        check_vma=False,
    )
```

```python
import math

import jax
import jax.numpy as jnp
from jax import lax
from jax.experimental import pallas as pl
from jax.experimental.pallas import tpu as pltpu
from jax.sharding import PartitionSpec as P

F32 = jnp.float32
BF16 = jnp.bfloat16
MESH = pl.DeviceIdType.MESH

SIGMA_SCALE = 0.5 * 4.0 ** (-1.0 / 6.0)
CHARGE_SCALE = math.sqrt(0.1 / math.sqrt(2.0))
FORCE_SCALE = 12.0 * math.sqrt(0.5)
CENTRE = 4
LEAVE_CENTRE = 7
CHUNK = 16
LATE_A, LATE_B = 14, 20


def split3(x):
    high = x.astype(BF16)
    rest = x - high.astype(F32)
    mid = rest.astype(BF16)
    low = (rest - mid.astype(F32)).astype(BF16)
    return high, mid, low


def join3(x):
    return x[0:8] + (x[8:16] + x[16:24])


def pair(own, other):
    dx, dy, dz = own[0] - other[0], own[1] - other[1], own[2] - other[2]
    r2 = dx * dx + dy * dy + dz * dz
    c = jnp.maximum(own[6], other[6])
    h = own[3] + other[3]
    h2 = h * h
    s = h2 * h2 * h2
    r4 = r2 * r2
    inverse = 1.0 / (s * c + r4 * r2)
    u = s * inverse
    root = lax.rsqrt(c + r2)
    t = (own[4] * other[4]) * u
    ty = t * (u - 1.0)
    coul = (own[5] * other[5]) * root
    return (dx, dy, dz), c, r4, inverse, u, root, t, ty, coul


def kernel(
    sizes,
    frac_hbm,
    type_hbm,
    pert_hbm,
    leaving_hbm,
    neighbours_hbm,
    counts_hbm,
    sigma_hbm,
    depth_hbm,
    charge_hbm,
    edge_hbm,
    coupling_hbm,
    forces_out,
    energy_hbm,
    dhdl_hbm,
    energy_out,
    dhdl_out,
    leaving,
    neighbours,
    counts,
    sigma_table,
    depth_table,
    charge_table,
    edge,
    coupling,
    kinds,
    rows_in,
    table,
    raw,
    leavers,
    landed,
    theirs,
    ghost,
    own,
    force_acc,
    plane_sums,
    line_sums,
    in_sem,
    rows_sem,
    ici_send,
    leave_recv,
    halo_recv,
    over_recv,
    plane_send,
    plane_recv,
    line_send,
    line_recv,
    out_sem,
    token,
):
    n_dx, n_dy, n_dz, blocks, listed = sizes
    me_x, me_y, me_z = lax.axis_index("dx"), lax.axis_index("dy"), lax.axis_index("dz")

    def along(a, b, c=0):
        return {
            "dx": lax.rem(me_x + a % n_dx, n_dx),
            "dy": lax.rem(me_y + b % n_dy, n_dy),
            "dz": lax.rem(me_z + c, n_dz),
        }

    def signal(semaphore, device):
        pl.semaphore_signal(semaphore, inc=1, device_id=device, device_id_type=MESH)

    copies = [
        (leaving_hbm, leaving),
        (sigma_hbm, sigma_table),
        (depth_hbm, depth_table),
        (charge_hbm, charge_table),
        (coupling_hbm, coupling),
        (edge_hbm, edge),
        (neighbours_hbm, neighbours),
        (counts_hbm, counts),
    ]
    copies = [
        pltpu.make_async_copy(src, dst, in_sem.at[i]) for i, (src, dst) in enumerate(copies)
    ]
    for copy in copies:
        copy.start()
    for q in range(blocks):
        lanes = pl.ds(q * 128, 128)
        row_copies = [(frac_hbm.at[k, 0, 0, 0, lanes], raw.at[CENTRE, q, k]) for k in range(3)]
        row_copies.append((type_hbm.at[0, 0, 0, lanes], kinds.at[q]))
        row_copies.append((pert_hbm.at[0, 0, 0, lanes], kinds.at[blocks + q]))
        for src, dst in row_copies:
            pltpu.make_async_copy(src, dst, rows_sem).start()

    def wait_bytes(ref, semaphore):
        pltpu.make_async_copy(ref, ref, semaphore).wait()

    peers = [(b, c) for b in range(n_dy) for c in range(n_dz) if (b, c) != (0, 0)]
    near = [(a, b, 0) for a in (1, -1, 2, -2) for b in (0, 1, -1)]
    near += [(0, b, c) for b, c in peers]
    barrier = pltpu.get_barrier_semaphore()
    for device in near:
        signal(barrier, along(*device))

    row8 = lax.broadcasted_iota(jnp.int32, (8, 128), 0)
    lane8 = lax.broadcasted_iota(jnp.int32, (8, 128), 1)
    for copy in copies:
        copy.wait()
    wait_bytes(rows_in.at[pl.ds(0, 5 * blocks)], rows_sem)
    lam = coupling[0]
    center = 13 * blocks

    def block_number(q, e):
        used = e < counts[0, 0, 0, q]
        return jnp.where(used, neighbours[0, 0, q, 0, e], 27 * blocks)

    leave_slots = jnp.full((8, 128), -1, jnp.int32)
    land_slots = jnp.full((8, 128), -1, jnp.int32)
    for m in range(16):
        up, down = leaving[0, 0, 0, 0, m], leaving[0, 0, 0, 1, m]
        leave_slots = jnp.where(lane8 == m, down, jnp.where(lane8 == m + 16, up, leave_slots))
        land_slots = jnp.where(lane8 == m, up, jnp.where(lane8 == m + 16, down, land_slots))
    kind = kinds[0:blocks, :]
    sigma = jnp.zeros((blocks, 128), F32)
    depth = jnp.zeros((blocks, 128), F32)
    charge = jnp.zeros((blocks, 128), F32)
    for k in range(sigma_table.shape[0]):
        hit = kind == k
        sigma = jnp.where(hit, sigma_table[k], sigma)
        depth = jnp.where(hit, depth_table[k], depth)
        charge = jnp.where(hit, charge_table[k], charge)
    flag = kinds[blocks : 2 * blocks, :].astype(F32)
    table[0] = sigma * SIGMA_SCALE
    table[1] = jnp.sqrt(depth)
    table[2] = charge * CHARGE_SCALE
    table[3] = flag
    for q in range(blocks):
        for k in range(5):
            raw[CENTRE, q, 3 + k : 4 + k, :] = table[min(k, 3), q : q + 1, :]

    rows = lax.broadcasted_iota(jnp.int32, (128, 128), 0)
    gathered = jnp.zeros((24, 128), F32)
    for q in range(blocks):
        pick = (leave_slots[0:1] == rows + q * 128).astype(F32).astype(BF16)
        parts = jnp.concatenate(split3(raw[CENTRE, q]), axis=0)
        gathered += jnp.dot(parts, pick, preferred_element_type=F32)
    leavers[LEAVE_CENTRE] = jnp.where(row8 == 7, land_slots.astype(F32), join3(gathered))

    pl.semaphore_wait(barrier, len(near))
    leaves, halos = {}, {}
    for a in (1, -1, 2, -2, 0):
        for b in (0, 1, -1):
            if (a, b) != (0, 0):
                i = 3 * (a + 2) + b + 1
                leaves[a, b] = pltpu.make_async_remote_copy(
                    leavers.at[LEAVE_CENTRE],
                    leavers.at[i],
                    ici_send,
                    leave_recv,
                    along(-a, -b),
                    MESH,
                )
                leaves[a, b].start()
    for a, b in ((-1, 0), (1, 0), (0, 1), (0, -1), (1, 1), (-1, 1), (1, -1), (-1, -1)):
        i = 3 * (a + 1) + b + 1
        halos[a, b] = pltpu.make_async_remote_copy(
            raw.at[CENTRE],
            raw.at[i],
            ici_send,
            halo_recv,
            along(-a, -b),
            MESH,
        )
        halos[a, b].start()
    for a in (-2, 2):
        signal(token.at[0], along(a, 0))

    spacing = float(blocks * 128) ** (1.0 / 3.0) * math.sqrt(0.5)
    scale = jnp.ones((8, 128), F32)
    for k in range(3):
        scale = jnp.where(row8 == k, edge[k] * spacing, scale)
    scale = jnp.where(row8 == 6, 0.25 * lam, jnp.where(row8 == 7, -lam, scale))
    base = jnp.where(row8 == 6, 0.15, jnp.where(row8 == 7, 1.0, 0.0))
    step_z = jnp.where(row8 == 2, scale, 0.0)
    lane32 = lax.broadcasted_iota(jnp.int32, (32, 128), 1).astype(F32)
    step_x = jnp.where(row8 == 0, jnp.where(lane8 < 16, 1.0, -1.0), 0.0)
    ones8 = jnp.ones((8, 128), BF16)
    ghost[27 * blocks] = jnp.where(
        row8 == 3, 1.0, jnp.where(row8 == 6, 0.15, jnp.where(row8 == 7, 1.0, 0.0))
    )
    itself = []
    for q in range(blocks):
        times = jnp.int32(0)
        for e in range(listed):
            times += jnp.where(block_number(q, e) == center + q, 1, 0)
        itself.append(jnp.full((1, 128), times, jnp.int32).astype(F32))
    around = ((0, 0), (0, 1), (0, -1), (-1, 0), (1, 0), (-1, 1), (1, 1), (-1, -1), (1, -1))
    wait_bytes(leavers.at[pl.ds(0, len(leaves))], leave_recv)

    for a, b in around:
        i = 3 * (a + 1) + b + 1
        here, above, below = (leavers[3 * (a + 2 + k) + b + 1] for k in (0, 1, -1))
        slots = jnp.broadcast_to(here.T[0:32, 7:8], (32, 128))
        tile = jnp.where(lane8 < 16, above, below) + step_x
        tile = jnp.where(row8 == 7, pltpu.roll(tile, 1, 0), tile)
        parts = jnp.concatenate((*split3(tile), ones8), axis=0)
        for q in range(blocks):
            spread = (slots == lane32 + float(q * 128)).astype(F32).astype(BF16)
            arrived = jnp.dot(parts[:, 0:32], spread, preferred_element_type=F32)
            landed[i, q, 0:8] = join3(arrived)
            landed[i, q, 8:16] = arrived[24:32]

    wait_bytes(raw.at[pl.ds(0, len(halos))], halo_recv)
    for a, b in around:
        i = 3 * (a + 1) + b + 1
        offset = base
        for k, value in enumerate((a, b)):
            if value:
                offset = jnp.where(row8 == k, scale * float(value), offset)
        for q in range(blocks):
            moved = jnp.where(landed[i, q, 8:16] > 0.5, landed[i, q, 0:8], raw[i, q])
            ghost[(3 * i + 1) * blocks + q] = moved * scale + offset
        over = pltpu.make_async_remote_copy(
            ghost.at[pl.ds((3 * i + 1) * blocks, blocks)],
            theirs.at[i],
            ici_send,
            over_recv,
            along(0, 0, 1),
            MESH,
        )
        over.start()

    pl.semaphore_wait(token.at[0], 2)
    for a in (-4, 4):
        signal(token.at[1], along(a, 0))
    self_sums = [jnp.zeros((1, 128), F32)] * 3
    for q in range(blocks):
        tile = ghost[center + q]
        columns = tile.T
        for k in range(8):
            own[k, q * 128 : q * 128 + 128, :] = jnp.broadcast_to(
                columns[:, k : k + 1], (128, 128)
            )
        atom = [tile[r : r + 1] for r in range(8)]
        _, _, _, _, u, root, t, ty, coul = pair(atom, atom)
        v = (ty - t) + coul
        g = u * ty + 0.25 * (coul * (root * root))
        off = 1.0 - atom[7]
        self_sums = [
            total + itself[q] * term for total, term in zip(self_sums, (v, off * v, off * g))
        ]

    wait_bytes(theirs, over_recv)
    for i in range(9):
        for q in range(blocks):
            for c in (-1, 1):
                ghost[(3 * i + 1 + c) * blocks + q] = theirs[i, q] + (step_z * float(c))

    steps = blocks * 128 // CHUNK
    per_block = 128 // CHUNK
    halves = CHUNK // 8

    def pair_step(with_energy, with_force):
        def step(k, sums):
            q = k // per_block
            atoms = [
                [own[r, pl.ds(k * CHUNK + 8 * half, 8), :] for r in range(8)]
                for half in range(halves)
            ]
            force = [[jnp.zeros((8, 128), F32)] * 3 for _ in atoms]
            for e in range(listed):
                number = block_number(q, e)
                other = [ghost[number, r : r + 1, :] for r in range(8)]
                for half, atom in enumerate(atoms):
                    d, _, r4, inverse, u, root, t, ty, coul = pair(atom, other)
                    w = jnp.minimum(atom[7], other[7])
                    m = coul * (root * root)
                    if with_energy:
                        v_sum, ov_sum, og_sum = sums
                        off = 1.0 - w
                        v = (ty - t) + coul
                        g = u * ty + 0.25 * m
                        sums = v_sum + v, ov_sum + off * v, og_sum + off * g
                    if with_force:
                        f = ((r4 * inverse) * ty + m * (1.0 / 12.0)) * w
                        force[half] = [total + f * part for total, part in zip(force[half], d)]
            if with_force:
                for half, totals in enumerate(force):
                    for axis, total in enumerate(totals):
                        force_acc[axis, pl.ds(k * CHUNK + 8 * half, 8), :] = total
            return sums

        return step

    zero = jnp.zeros((8, 128), F32)
    both = steps - LATE_A - LATE_B
    sums = lax.fori_loop(0, both, pair_step(True, True), (zero, zero, zero))
    pl.semaphore_wait(token.at[1], 2)
    for a in (-8, 8):
        signal(token.at[2], along(a, 0))
    sums = lax.fori_loop(both, steps, pair_step(True, False), sums)
    v_row, ov_row, og_row = (
        jnp.sum(total, axis=0, keepdims=True) - itself for total, itself in zip(sums, self_sums)
    )
    lane1 = lax.broadcasted_iota(jnp.int32, (1, 128), 1)
    energy_row = v_row - ov_row
    dhdl_row = ov_row + (0.5 * (1.0 - lam)) * og_row
    energy_row += pltpu.roll(energy_row, 64, 1)
    dhdl_row += pltpu.roll(dhdl_row, 64, 1)
    part = jnp.where(lane1 < 64, energy_row, dhdl_row)

    my_peer = me_y * n_dz + me_z
    plane_sums[my_peer] = part
    plane_copies = []
    for i, (b, c) in enumerate(peers):
        plane_copies.append(
            pltpu.make_async_remote_copy(
                plane_sums.at[my_peer],
                plane_sums.at[my_peer],
                plane_send,
                plane_recv,
                along(0, b, c),
                MESH,
            )
        )
    for copy in plane_copies:
        copy.start()

    lax.fori_loop(both, both + LATE_A, pair_step(False, True), ())
    ones = jnp.ones((8, 384), BF16)

    def row_sums(axis):
        for q in range(blocks):
            parts = jnp.concatenate(
                split3(force_acc[axis, q * 128 : q * 128 + 128, :]), axis=1
            )
            total = lax.dot_general(
                ones, parts, (((1,), (1,)), ((), ())), preferred_element_type=F32
            )
            forces_out[axis, 0, 0, :, q * 128 : q * 128 + 128] = total[0:1] * FORCE_SCALE

    wait_bytes(plane_sums.at[pl.ds(0, len(peers))], plane_recv)
    total = plane_sums[0]
    for i in range(1, n_dy * n_dz):
        total = total + plane_sums[i]
    line_sums[me_x] = total
    pl.semaphore_wait(token.at[2], 2)
    line_copies = []
    for d in sorted(range(1, n_dx), key=lambda d: min(d, n_dx - d)):
        line_copies.append(
            pltpu.make_async_remote_copy(
                line_sums.at[me_x],
                line_sums.at[me_x],
                line_send,
                line_recv,
                along(d, 0),
                MESH,
            )
        )
    for copy in line_copies:
        copy.start()
    lax.fori_loop(both + LATE_A, steps, pair_step(False, True), ())
    for axis in range(3):
        row_sums(axis)
    wait_bytes(line_sums.at[pl.ds(0, n_dx - 1)], line_recv)
    total = line_sums[0]
    for i in range(1, n_dx):
        total = total + line_sums[i]
    norm = 0.5 / (blocks * 128 * n_dx * n_dy * n_dz)
    energy_out[0] = jnp.sum(jnp.where(lane1 < 64, total, 0.0)) * norm
    dhdl_out[0] = jnp.sum(jnp.where(lane1 < 64, 0.0, total)) * (-norm / lam)
    results = [
        pltpu.make_async_copy(energy_out, energy_hbm, out_sem.at[0]),
        pltpu.make_async_copy(dhdl_out, dhdl_hbm, out_sem.at[1]),
    ]
    for copy in results:
        copy.start()
    wait_bytes(ghost.at[pl.ds(0, len(leaves) + (len(halos) + 9) * blocks)], ici_send)
    wait_bytes(plane_sums.at[pl.ds(0, len(peers))], plane_send)
    wait_bytes(line_sums.at[pl.ds(0, n_dx - 1)], line_send)
    for copy in results:
        copy.wait()


def on_device(
    fraction,
    atom_type,
    perturbed,
    leaving,
    neighbours,
    counts,
    sigma_table,
    depth_table,
    charge_table,
    domain_edge,
    coupling,
):
    n_dx, n_dy, n_dz = (lax.axis_size(axis) for axis in ("dx", "dy", "dz"))
    atoms = fraction.shape[-1]
    blocks = atoms // 128
    sizes = (n_dx, n_dy, n_dz, blocks, neighbours.shape[-1])
    neighbours = neighbours.transpose(0, 1, 3, 2, 4)
    hbm = pl.BlockSpec(memory_space=pltpu.HBM)
    dma, regular = pltpu.SemaphoreType.DMA, pltpu.SemaphoreType.REGULAR
    scalars = (
        leaving,
        neighbours,
        counts,
        sigma_table,
        depth_table,
        charge_table,
        domain_edge,
        coupling,
    )
    return pl.pallas_call(
        lambda *refs: kernel(sizes, *refs),
        out_shape=(
            pltpu.VMEM(fraction.shape, F32),
            jax.ShapeDtypeStruct((1,), F32),
            jax.ShapeDtypeStruct((1,), F32),
        ),
        in_specs=[hbm] * 11,
        out_specs=(pl.BlockSpec(memory_space=pltpu.VMEM), hbm, hbm),
        scratch_shapes=[
            pltpu.SMEM((1,), F32),
            pltpu.SMEM((1,), F32),
            *[pltpu.SMEM(array.shape, array.dtype) for array in scalars],
            pltpu.VMEM((2 * blocks, 128), jnp.int32),
            pltpu.VMEM((5 * blocks, 128), F32),
            pltpu.VMEM((4, blocks, 128), F32),
            pltpu.VMEM((9, blocks, 8, 128), F32),
            pltpu.VMEM((15, 8, 128), F32),
            pltpu.VMEM((9, blocks, 16, 128), F32),
            pltpu.VMEM((9, blocks, 8, 128), F32),
            pltpu.VMEM((27 * blocks + 1, 8, 128), F32),
            pltpu.VMEM((8, atoms, 128), F32),
            pltpu.VMEM((3, atoms, 128), F32),
            pltpu.VMEM((n_dy * n_dz, 1, 128), F32),
            pltpu.VMEM((n_dx, 1, 128), F32),
            dma((len(scalars),)),
            *[dma] * 9,
            dma((2,)),
            regular((3,)),
        ],
        compiler_params=pltpu.CompilerParams(
            collective_id=0, has_side_effects=True, vmem_limit_bytes=62 * 1024 * 1024
        ),
        name="step",
    )(
        fraction,
        atom_type,
        perturbed,
        leaving,
        neighbours,
        counts,
        sigma_table,
        depth_table,
        charge_table,
        domain_edge,
        coupling,
    )


def solution(mesh):
    return jax.shard_map(
        on_device,
        mesh=mesh,
        in_specs=(
            P(None, ("win", "dx"), "dy", "dz", None),
            P(("win", "dx"), "dy", "dz", None),
            P(("win", "dx"), "dy", "dz", None),
            P(("win", "dx"), "dy", "dz", None, None),
            P(("win", "dx"), "dy", "dz", None, None),
            P(("win", "dx"), "dy", "dz", None),
            P(),
            P(),
            P(),
            P(),
            P("win"),
        ),
        out_specs=(P(None, ("win", "dx"), "dy", "dz", None), P("win"), P("win")),
        check_vma=False,
    )
```

```python
import math

import jax
import jax.numpy as jnp
from jax import lax
from jax.experimental import pallas as pl
from jax.experimental.pallas import tpu as pltpu
from jax.sharding import PartitionSpec as P

F32 = jnp.float32
BF16 = jnp.bfloat16
MESH = pl.DeviceIdType.MESH

SIGMA_SCALE = 0.5 * 4.0 ** (-1.0 / 6.0)
CHARGE_SCALE = math.sqrt(0.1 / math.sqrt(2.0))
FORCE_SCALE = 12.0 * math.sqrt(0.5)
CENTRE = 4
LEAVE_CENTRE = 7
CHUNK = 16
LATE_A, LATE_B = 14, 20


def split3(x):
    high = x.astype(BF16)
    rest = x - high.astype(F32)
    mid = rest.astype(BF16)
    low = (rest - mid.astype(F32)).astype(BF16)
    return high, mid, low


def join3(x):
    return x[0:8] + (x[8:16] + x[16:24])


def pair(own, other):
    dx, dy, dz = own[0] - other[0], own[1] - other[1], own[2] - other[2]
    r2 = dx * dx + dy * dy + dz * dz
    c = jnp.maximum(own[6], other[6])
    h = own[3] + other[3]
    h2 = h * h
    s = h2 * h2 * h2
    r4 = r2 * r2
    inverse = 1.0 / (s * c + r4 * r2)
    u = s * inverse
    root = lax.rsqrt(c + r2)
    t = (own[4] * other[4]) * u
    ty = t * (u - 1.0)
    coul = (own[5] * other[5]) * root
    return (dx, dy, dz), c, r4, inverse, u, root, t, ty, coul


def kernel(
    sizes,
    frac_hbm,
    type_hbm,
    pert_hbm,
    leaving_hbm,
    neighbours_hbm,
    counts_hbm,
    sigma_hbm,
    depth_hbm,
    charge_hbm,
    edge_hbm,
    coupling_hbm,
    forces_out,
    energy_hbm,
    dhdl_hbm,
    energy_out,
    dhdl_out,
    leaving,
    neighbours,
    counts,
    sigma_table,
    depth_table,
    charge_table,
    edge,
    coupling,
    kinds,
    rows_in,
    table,
    raw,
    leavers,
    landed,
    theirs,
    ghost,
    places,
    own,
    force_acc,
    plane_sums,
    line_sums,
    total_out,
    total_in,
    in_sem,
    rows_sem,
    ici_send,
    leave_recv,
    halo_recv,
    over_recv,
    plane_send,
    plane_recv,
    line_send,
    line_recv,
    total_send,
    total_recv,
    out_sem,
    token,
):
    n_dx, n_dy, n_dz, blocks, listed = sizes
    me_x, me_y, me_z = lax.axis_index("dx"), lax.axis_index("dy"), lax.axis_index("dz")

    def along(a, b, c=0):
        return {
            "dx": lax.rem(me_x + a % n_dx, n_dx),
            "dy": lax.rem(me_y + b % n_dy, n_dy),
            "dz": lax.rem(me_z + c, n_dz),
        }

    def signal(semaphore, device):
        pl.semaphore_signal(semaphore, inc=1, device_id=device, device_id_type=MESH)

    copies = [
        (leaving_hbm, leaving),
        (sigma_hbm, sigma_table),
        (depth_hbm, depth_table),
        (charge_hbm, charge_table),
        (coupling_hbm, coupling),
        (edge_hbm, edge),
        (neighbours_hbm, neighbours),
        (counts_hbm, counts),
    ]
    copies = [
        pltpu.make_async_copy(src, dst, in_sem.at[i]) for i, (src, dst) in enumerate(copies)
    ]
    for copy in copies:
        copy.start()
    for q in range(blocks):
        lanes = pl.ds(q * 128, 128)
        row_copies = [(frac_hbm.at[k, 0, 0, 0, lanes], raw.at[CENTRE, q, k]) for k in range(3)]
        row_copies.append((type_hbm.at[0, 0, 0, lanes], kinds.at[q]))
        row_copies.append((pert_hbm.at[0, 0, 0, lanes], kinds.at[blocks + q]))
        for src, dst in row_copies:
            pltpu.make_async_copy(src, dst, rows_sem).start()

    def wait_bytes(ref, semaphore):
        pltpu.make_async_copy(ref, ref, semaphore).wait()

    peers = [(b, c) for b in range(n_dy) for c in range(n_dz) if (b, c) != (0, 0)]
    near = [(a, b, 0) for a in (1, -1, 2, -2) for b in (0, 1, -1)]
    near += [(0, b, c) for b, c in peers]
    barrier = pltpu.get_barrier_semaphore()
    for device in near:
        signal(barrier, along(*device))

    row8 = lax.broadcasted_iota(jnp.int32, (8, 128), 0)
    lane8 = lax.broadcasted_iota(jnp.int32, (8, 128), 1)
    for copy in copies:
        copy.wait()
    wait_bytes(rows_in.at[pl.ds(0, 5 * blocks)], rows_sem)
    lam = coupling[0]
    plane = 9 * blocks
    center = plane + CENTRE * blocks

    leave_slots = jnp.full((8, 128), -1, jnp.int32)
    land_slots = jnp.full((8, 128), -1, jnp.int32)
    for m in range(16):
        up, down = leaving[0, 0, 0, 0, m], leaving[0, 0, 0, 1, m]
        leave_slots = jnp.where(lane8 == m, down, jnp.where(lane8 == m + 16, up, leave_slots))
        land_slots = jnp.where(lane8 == m, up, jnp.where(lane8 == m + 16, down, land_slots))
    kind = kinds[0:blocks, :]
    sigma = jnp.zeros((blocks, 128), F32)
    depth = jnp.zeros((blocks, 128), F32)
    charge = jnp.zeros((blocks, 128), F32)
    for k in range(sigma_table.shape[0]):
        hit = kind == k
        sigma = jnp.where(hit, sigma_table[k], sigma)
        depth = jnp.where(hit, depth_table[k], depth)
        charge = jnp.where(hit, charge_table[k], charge)
    flag = kinds[blocks : 2 * blocks, :].astype(F32)
    table[0] = sigma * SIGMA_SCALE
    table[1] = jnp.sqrt(depth)
    table[2] = charge * CHARGE_SCALE
    table[3] = flag
    for q in range(blocks):
        for k in range(5):
            raw[CENTRE, q, 3 + k : 4 + k, :] = table[min(k, 3), q : q + 1, :]

    rows = lax.broadcasted_iota(jnp.int32, (128, 128), 0)
    gathered = jnp.zeros((24, 128), F32)
    for q in range(blocks):
        pick = (leave_slots[0:1] == rows + q * 128).astype(F32).astype(BF16)
        parts = jnp.concatenate(split3(raw[CENTRE, q]), axis=0)
        gathered += jnp.dot(parts, pick, preferred_element_type=F32)
    leavers[LEAVE_CENTRE] = jnp.where(row8 == 7, land_slots.astype(F32), join3(gathered))

    pl.semaphore_wait(barrier, len(near))
    leaves, halos = {}, {}
    for a in (1, -1, 2, -2, 0):
        for b in (0, 1, -1):
            if (a, b) != (0, 0):
                i = 3 * (a + 2) + b + 1
                leaves[a, b] = pltpu.make_async_remote_copy(
                    leavers.at[LEAVE_CENTRE],
                    leavers.at[i],
                    ici_send,
                    leave_recv,
                    along(-a, -b),
                    MESH,
                )
                leaves[a, b].start()
    for a, b in ((-1, 0), (1, 0), (0, 1), (0, -1), (1, 1), (-1, 1), (1, -1), (-1, -1)):
        i = 3 * (a + 1) + b + 1
        halos[a, b] = pltpu.make_async_remote_copy(
            raw.at[CENTRE],
            raw.at[i],
            ici_send,
            halo_recv,
            along(-a, -b),
            MESH,
        )
        halos[a, b].start()
    for a in (-2, 2):
        signal(token.at[0], along(a, 0))

    spacing = float(blocks * 128) ** (1.0 / 3.0) * math.sqrt(0.5)
    scale = jnp.ones((8, 128), F32)
    for k in range(3):
        scale = jnp.where(row8 == k, edge[k] * spacing, scale)
    scale = jnp.where(row8 == 6, 0.25 * lam, jnp.where(row8 == 7, -lam, scale))
    base = jnp.where(row8 == 6, 0.15, jnp.where(row8 == 7, 1.0, 0.0))
    step_z = jnp.where(row8 == 2, scale, 0.0)
    lane32 = lax.broadcasted_iota(jnp.int32, (32, 128), 1).astype(F32)
    step_x = jnp.where(row8 == 0, jnp.where(lane8 < 16, 1.0, -1.0), 0.0)
    ones8 = jnp.ones((8, 128), BF16)
    ghost[27 * blocks] = jnp.where(
        row8 == 3, 1.0, jnp.where(row8 == 6, 0.15, jnp.where(row8 == 7, 1.0, 0.0))
    )
    itself = []
    for q in range(blocks):
        times = jnp.int32(0)
        for e in range(listed):
            number = neighbours[0, 0, q, 0, e]
            domain = number // blocks
            where = (domain % 3) * plane + (domain // 3) * blocks + number % blocks
            where = jnp.where(e < counts[0, 0, 0, q], where, 3 * plane)
            places[q * listed + e] = where
            times += jnp.where(where == center + q, 1, 0)
        itself.append(jnp.full((1, 128), times, jnp.int32).astype(F32))
    around = ((0, 0), (0, 1), (0, -1), (-1, 0), (1, 0), (-1, 1), (1, 1), (-1, -1), (1, -1))
    pl.semaphore_wait(token.at[0], 2)
    for a in (-4, 4):
        signal(token.at[1], along(a, 0))
    wait_bytes(leavers.at[pl.ds(0, len(leaves))], leave_recv)

    for a, b in around:
        i = 3 * (a + 1) + b + 1
        here, above, below = (leavers[3 * (a + 2 + k) + b + 1] for k in (0, 1, -1))
        slots = jnp.broadcast_to(here.T[0:32, 7:8], (32, 128))
        tile = jnp.where(lane8 < 16, above, below) + step_x
        tile = jnp.where(row8 == 7, pltpu.roll(tile, 1, 0), tile)
        parts = jnp.concatenate((*split3(tile), ones8), axis=0)
        for q in range(blocks):
            spread = (slots == lane32 + float(q * 128)).astype(F32).astype(BF16)
            arrived = jnp.dot(parts[:, 0:32], spread, preferred_element_type=F32)
            landed[i, q, 0:8] = join3(arrived)
            landed[i, q, 8:16] = arrived[24:32]

    wait_bytes(raw.at[pl.ds(0, len(halos))], halo_recv)
    for a, b in around:
        i = 3 * (a + 1) + b + 1
        offset = base
        for k, value in enumerate((a, b)):
            if value:
                offset = jnp.where(row8 == k, scale * float(value), offset)
        for q in range(blocks):
            moved = jnp.where(landed[i, q, 8:16] > 0.5, landed[i, q, 0:8], raw[i, q])
            ghost[plane + i * blocks + q] = moved * scale + offset
    pltpu.make_async_remote_copy(
        ghost.at[pl.ds(plane, plane)], theirs, ici_send, over_recv, along(0, 0, 1), MESH
    ).start()
    self_sums = [jnp.zeros((1, 128), F32)] * 3
    for q in range(blocks):
        tile = ghost[center + q]
        columns = tile.T
        for k in range(8):
            own[k, q * 128 : q * 128 + 128, :] = jnp.broadcast_to(
                columns[:, k : k + 1], (128, 128)
            )
        atom = [tile[r : r + 1] for r in range(8)]
        _, _, _, _, u, root, t, ty, coul = pair(atom, atom)
        v = (ty - t) + coul
        g = u * ty + 0.25 * (coul * (root * root))
        off = 1.0 - atom[7]
        self_sums = [
            total + itself[q] * term for total, term in zip(self_sums, (v, off * v, off * g))
        ]

    wait_bytes(theirs, over_recv)
    for i in range(plane):
        tile = theirs[i]
        ghost[i] = tile - step_z
        ghost[2 * plane + i] = tile + step_z

    steps = blocks * 128 // CHUNK
    per_block = 128 // CHUNK
    halves = CHUNK // 8

    def pair_step(with_energy, with_force):
        def step(k, sums):
            q = k // per_block
            atoms = [
                [own[r, pl.ds(k * CHUNK + 8 * half, 8), :] for r in range(8)]
                for half in range(halves)
            ]
            force = [[jnp.zeros((8, 128), F32)] * 3 for _ in atoms]
            for e in range(listed):
                place = places[q * listed + e]
                other = [ghost[place, r : r + 1, :] for r in range(8)]
                for half, atom in enumerate(atoms):
                    d, _, r4, inverse, u, root, t, ty, coul = pair(atom, other)
                    w = jnp.minimum(atom[7], other[7])
                    m = coul * (root * root)
                    if with_energy:
                        v_sum, ov_sum, og_sum = sums
                        off = 1.0 - w
                        v = (ty - t) + coul
                        g = u * ty + 0.25 * m
                        sums = v_sum + v, ov_sum + off * v, og_sum + off * g
                    if with_force:
                        f = ((r4 * inverse) * ty + m * (1.0 / 12.0)) * w
                        force[half] = [total + f * part for total, part in zip(force[half], d)]
            if with_force:
                for half, totals in enumerate(force):
                    for axis, total in enumerate(totals):
                        force_acc[axis, pl.ds(k * CHUNK + 8 * half, 8), :] = total
            return sums

        return step

    zero = jnp.zeros((8, 128), F32)
    both = steps - LATE_A - LATE_B
    sums = lax.fori_loop(0, both, pair_step(True, True), (zero, zero, zero))
    pl.semaphore_wait(token.at[1], 2)
    for a in (-8, 8):
        signal(token.at[2], along(a, 0))
    sums = lax.fori_loop(both, steps, pair_step(True, False), sums)
    v_row, ov_row, og_row = (
        jnp.sum(total, axis=0, keepdims=True) - itself for total, itself in zip(sums, self_sums)
    )
    lane1 = lax.broadcasted_iota(jnp.int32, (1, 128), 1)
    energy_row = v_row - ov_row
    dhdl_row = ov_row + (0.5 * (1.0 - lam)) * og_row
    energy_row += pltpu.roll(energy_row, 64, 1)
    dhdl_row += pltpu.roll(dhdl_row, 64, 1)
    part = jnp.where(lane1 < 64, energy_row, dhdl_row)

    leader = me_z == n_dz - 1
    my_peer = me_y * n_dz + me_z
    plane_sums[my_peer] = part

    def send_part(b, c):
        pltpu.make_async_remote_copy(
            plane_sums.at[my_peer],
            plane_sums.at[my_peer],
            plane_send,
            plane_recv,
            along(0, b, c),
            MESH,
        ).start()

    @pl.when(jnp.logical_not(leader))
    def _():
        for b in (0, 1, -1, 2):
            send_part(b, 1)

    @pl.when(leader)
    def _():
        for b in (1, -1, 2):
            send_part(b, 0)

    lax.fori_loop(both, both + LATE_A, pair_step(False, True), ())
    ones = jnp.ones((8, 384), BF16)

    def row_sums(axis):
        for q in range(blocks):
            parts = jnp.concatenate(
                split3(force_acc[axis, q * 128 : q * 128 + 128, :]), axis=1
            )
            total = lax.dot_general(
                ones, parts, (((1,), (1,)), ((), ())), preferred_element_type=F32
            )
            forces_out[axis, 0, 0, :, q * 128 : q * 128 + 128] = total[0:1] * FORCE_SCALE

    @pl.when(leader)
    def _():
        wait_bytes(plane_sums.at[pl.ds(0, len(peers))], plane_recv)
        total = plane_sums[0]
        for i in range(1, n_dy * n_dz):
            total = total + plane_sums[i]
        line_sums[me_x] = total
        pl.semaphore_wait(token.at[2], 2)
        for d in sorted(range(1, n_dx), key=lambda d: min(d, n_dx - d)):
            pltpu.make_async_remote_copy(
                line_sums.at[me_x],
                line_sums.at[me_x],
                line_send,
                line_recv,
                along(d, 0),
                MESH,
            ).start()

    @pl.when(jnp.logical_not(leader))
    def _():
        pl.semaphore_wait(token.at[2], 2)

    lax.fori_loop(both + LATE_A, steps, pair_step(False, True), ())
    for axis in range(3):
        row_sums(axis)
    @pl.when(leader)
    def _():
        wait_bytes(line_sums.at[pl.ds(0, n_dx - 1)], line_recv)
        total = line_sums[0]
        for i in range(1, n_dx):
            total = total + line_sums[i]
        total_out[...] = total
        pltpu.make_async_remote_copy(
            total_out, total_in, total_send, total_recv, along(0, 0, 1), MESH
        ).start()

    @pl.when(jnp.logical_not(leader))
    def _():
        wait_bytes(total_in, total_recv)
        total_out[...] = total_in[...]

    total = total_out[...]
    norm = 0.5 / (blocks * 128 * n_dx * n_dy * n_dz)
    energy_out[0] = jnp.sum(jnp.where(lane1 < 64, total, 0.0)) * norm
    dhdl_out[0] = jnp.sum(jnp.where(lane1 < 64, 0.0, total)) * (-norm / lam)
    results = [
        pltpu.make_async_copy(energy_out, energy_hbm, out_sem.at[0]),
        pltpu.make_async_copy(dhdl_out, dhdl_hbm, out_sem.at[1]),
    ]
    for copy in results:
        copy.start()
    wait_bytes(ghost.at[pl.ds(0, len(leaves) + (len(halos) + 9) * blocks)], ici_send)

    @pl.when(leader)
    def _():
        wait_bytes(plane_sums.at[pl.ds(0, n_dy - 1)], plane_send)
        wait_bytes(line_sums.at[pl.ds(0, n_dx - 1)], line_send)
        wait_bytes(total_out, total_send)

    @pl.when(jnp.logical_not(leader))
    def _():
        wait_bytes(plane_sums.at[pl.ds(0, n_dy)], plane_send)

    for copy in results:
        copy.wait()


def on_device(
    fraction,
    atom_type,
    perturbed,
    leaving,
    neighbours,
    counts,
    sigma_table,
    depth_table,
    charge_table,
    domain_edge,
    coupling,
):
    n_dx, n_dy, n_dz = (lax.axis_size(axis) for axis in ("dx", "dy", "dz"))
    atoms = fraction.shape[-1]
    blocks = atoms // 128
    sizes = (n_dx, n_dy, n_dz, blocks, neighbours.shape[-1])
    neighbours = neighbours.transpose(0, 1, 3, 2, 4)
    hbm = pl.BlockSpec(memory_space=pltpu.HBM)
    dma, regular = pltpu.SemaphoreType.DMA, pltpu.SemaphoreType.REGULAR
    scalars = (
        leaving,
        neighbours,
        counts,
        sigma_table,
        depth_table,
        charge_table,
        domain_edge,
        coupling,
    )
    return pl.pallas_call(
        lambda *refs: kernel(sizes, *refs),
        out_shape=(
            pltpu.VMEM(fraction.shape, F32),
            jax.ShapeDtypeStruct((1,), F32),
            jax.ShapeDtypeStruct((1,), F32),
        ),
        in_specs=[hbm] * 11,
        out_specs=(pl.BlockSpec(memory_space=pltpu.VMEM), hbm, hbm),
        scratch_shapes=[
            pltpu.SMEM((1,), F32),
            pltpu.SMEM((1,), F32),
            *[pltpu.SMEM(array.shape, array.dtype) for array in scalars],
            pltpu.VMEM((2 * blocks, 128), jnp.int32),
            pltpu.VMEM((5 * blocks, 128), F32),
            pltpu.VMEM((4, blocks, 128), F32),
            pltpu.VMEM((9, blocks, 8, 128), F32),
            pltpu.VMEM((15, 8, 128), F32),
            pltpu.VMEM((9, blocks, 16, 128), F32),
            pltpu.VMEM((9 * blocks, 8, 128), F32),
            pltpu.VMEM((27 * blocks + 1, 8, 128), F32),
            pltpu.SMEM((blocks * neighbours.shape[-1],), jnp.int32),
            pltpu.VMEM((8, atoms, 128), F32),
            pltpu.VMEM((3, atoms, 128), F32),
            pltpu.VMEM((n_dy * n_dz, 1, 128), F32),
            pltpu.VMEM((n_dx, 1, 128), F32),
            pltpu.VMEM((1, 128), F32),
            pltpu.VMEM((1, 128), F32),
            dma((len(scalars),)),
            *[dma] * 11,
            dma((2,)),
            regular((3,)),
        ],
        compiler_params=pltpu.CompilerParams(
            collective_id=0, has_side_effects=True, vmem_limit_bytes=62 * 1024 * 1024
        ),
        name="step",
    )(
        fraction,
        atom_type,
        perturbed,
        leaving,
        neighbours,
        counts,
        sigma_table,
        depth_table,
        charge_table,
        domain_edge,
        coupling,
    )


def solution(mesh):
    return jax.shard_map(
        on_device,
        mesh=mesh,
        in_specs=(
            P(None, ("win", "dx"), "dy", "dz", None),
            P(("win", "dx"), "dy", "dz", None),
            P(("win", "dx"), "dy", "dz", None),
            P(("win", "dx"), "dy", "dz", None, None),
            P(("win", "dx"), "dy", "dz", None, None),
            P(("win", "dx"), "dy", "dz", None),
            P(),
            P(),
            P(),
            P(),
            P("win"),
        ),
        out_specs=(P(None, ("win", "dx"), "dy", "dz", None), P("win"), P("win")),
        check_vma=False,
    )
```

```python
import math

import jax
import jax.numpy as jnp
from jax import lax
from jax.experimental import pallas as pl
from jax.experimental.pallas import tpu as pltpu
from jax.sharding import PartitionSpec as P

F32 = jnp.float32
BF16 = jnp.bfloat16
MESH = pl.DeviceIdType.MESH

SIGMA_SCALE = 0.5 * 4.0 ** (-1.0 / 6.0)
CHARGE_SCALE = math.sqrt(0.1 / math.sqrt(2.0))
FORCE_SCALE = 12.0 * math.sqrt(0.5)
CENTRE = 4
LEAVE_CENTRE = 7
CHUNK = 16
WIDE = 32
LATE_A, LATE_B = 18, 18


def split3(x):
    high = x.astype(BF16)
    rest = x - high.astype(F32)
    mid = rest.astype(BF16)
    low = (rest - mid.astype(F32)).astype(BF16)
    return high, mid, low


def join3(x):
    return x[0:8] + (x[8:16] + x[16:24])


def pair(own, other):
    dx, dy, dz = own[0] - other[0], own[1] - other[1], own[2] - other[2]
    r2 = dx * dx + dy * dy + dz * dz
    c = jnp.maximum(own[6], other[6])
    h = own[3] + other[3]
    h2 = h * h
    s = h2 * h2 * h2
    r4 = r2 * r2
    inverse = 1.0 / (s * c + r4 * r2)
    u = s * inverse
    root = lax.rsqrt(c + r2)
    t = (own[4] * other[4]) * u
    ty = t * (u - 1.0)
    coul = (own[5] * other[5]) * root
    return (dx, dy, dz), c, r4, inverse, u, root, t, ty, coul


def kernel(
    sizes,
    frac_hbm,
    type_hbm,
    pert_hbm,
    leaving_hbm,
    neighbours_hbm,
    counts_hbm,
    sigma_hbm,
    depth_hbm,
    charge_hbm,
    edge_hbm,
    coupling_hbm,
    forces_out,
    energy_hbm,
    dhdl_hbm,
    energy_out,
    dhdl_out,
    leaving,
    neighbours,
    counts,
    sigma_table,
    depth_table,
    charge_table,
    edge,
    coupling,
    kinds,
    rows_in,
    table,
    raw,
    leavers,
    landed,
    theirs,
    ghost,
    places,
    own,
    force_acc,
    plane_sums,
    line_sums,
    total_out,
    total_in,
    in_sem,
    rows_sem,
    ici_send,
    leave_recv,
    halo_recv,
    over_recv,
    plane_send,
    plane_recv,
    line_send,
    line_recv,
    total_send,
    total_recv,
    out_sem,
    token,
):
    n_dx, n_dy, n_dz, blocks, listed = sizes
    me_x, me_y, me_z = lax.axis_index("dx"), lax.axis_index("dy"), lax.axis_index("dz")

    def along(a, b, c=0):
        return {
            "dx": lax.rem(me_x + a % n_dx, n_dx),
            "dy": lax.rem(me_y + b % n_dy, n_dy),
            "dz": lax.rem(me_z + c, n_dz),
        }

    def signal(semaphore, device):
        pl.semaphore_signal(semaphore, inc=1, device_id=device, device_id_type=MESH)

    copies = [
        (leaving_hbm, leaving),
        (sigma_hbm, sigma_table),
        (depth_hbm, depth_table),
        (charge_hbm, charge_table),
        (coupling_hbm, coupling),
        (edge_hbm, edge),
        (neighbours_hbm, neighbours),
        (counts_hbm, counts),
    ]
    copies = [
        pltpu.make_async_copy(src, dst, in_sem.at[i]) for i, (src, dst) in enumerate(copies)
    ]
    for copy in copies:
        copy.start()
    for q in range(blocks):
        lanes = pl.ds(q * 128, 128)
        row_copies = [(frac_hbm.at[k, 0, 0, 0, lanes], raw.at[CENTRE, q, k]) for k in range(3)]
        row_copies.append((type_hbm.at[0, 0, 0, lanes], kinds.at[q]))
        row_copies.append((pert_hbm.at[0, 0, 0, lanes], kinds.at[blocks + q]))
        for src, dst in row_copies:
            pltpu.make_async_copy(src, dst, rows_sem).start()

    def wait_bytes(ref, semaphore):
        pltpu.make_async_copy(ref, ref, semaphore).wait()

    peers = [(b, c) for b in range(n_dy) for c in range(n_dz) if (b, c) != (0, 0)]
    near = [(a, b, 0) for a in (2, -2, 1, -1) for b in (1, -1, 0)]
    near += [(0, b, c) for b, c in peers]
    barrier = pltpu.get_barrier_semaphore()
    for device in near:
        signal(barrier, along(*device))

    row8 = lax.broadcasted_iota(jnp.int32, (8, 128), 0)
    lane8 = lax.broadcasted_iota(jnp.int32, (8, 128), 1)
    for copy in copies:
        copy.wait()
    wait_bytes(rows_in.at[pl.ds(0, 5 * blocks)], rows_sem)
    lam = coupling[0]
    plane = 9 * blocks
    center = plane + CENTRE * blocks

    leave_slots = jnp.full((8, 128), -1, jnp.int32)
    land_slots = jnp.full((8, 128), -1, jnp.int32)
    for m in range(16):
        up, down = leaving[0, 0, 0, 0, m], leaving[0, 0, 0, 1, m]
        leave_slots = jnp.where(lane8 == m, down, jnp.where(lane8 == m + 16, up, leave_slots))
        land_slots = jnp.where(lane8 == m, up, jnp.where(lane8 == m + 16, down, land_slots))
    kind = kinds[0:blocks, :]
    sigma = jnp.zeros((blocks, 128), F32)
    depth = jnp.zeros((blocks, 128), F32)
    charge = jnp.zeros((blocks, 128), F32)
    for k in range(sigma_table.shape[0]):
        hit = kind == k
        sigma = jnp.where(hit, sigma_table[k], sigma)
        depth = jnp.where(hit, depth_table[k], depth)
        charge = jnp.where(hit, charge_table[k], charge)
    flag = kinds[blocks : 2 * blocks, :].astype(F32)
    table[0] = sigma * SIGMA_SCALE
    table[1] = jnp.sqrt(depth)
    table[2] = charge * CHARGE_SCALE
    table[3] = flag
    for q in range(blocks):
        for k in range(5):
            raw[CENTRE, q, 3 + k : 4 + k, :] = table[min(k, 3), q : q + 1, :]

    rows = lax.broadcasted_iota(jnp.int32, (128, 128), 0)
    gathered = jnp.zeros((24, 128), F32)
    for q in range(blocks):
        pick = (leave_slots[0:1] == rows + q * 128).astype(F32).astype(BF16)
        parts = jnp.concatenate(split3(raw[CENTRE, q]), axis=0)
        gathered += jnp.dot(parts, pick, preferred_element_type=F32)
    leavers[LEAVE_CENTRE] = jnp.where(row8 == 7, land_slots.astype(F32), join3(gathered))

    pl.semaphore_wait(barrier, len(near))
    leaves, halos = {}, {}
    for a in (2, -2, 1, -1, 0):
        for b in (1, -1, 0):
            if (a, b) != (0, 0):
                i = 3 * (a + 2) + b + 1
                leaves[a, b] = pltpu.make_async_remote_copy(
                    leavers.at[LEAVE_CENTRE],
                    leavers.at[i],
                    ici_send,
                    leave_recv,
                    along(-a, -b),
                    MESH,
                )
                leaves[a, b].start()
    for a, b in ((-1, 0), (1, 0), (0, 1), (0, -1), (1, 1), (-1, 1), (1, -1), (-1, -1)):
        i = 3 * (a + 1) + b + 1
        halos[a, b] = pltpu.make_async_remote_copy(
            raw.at[CENTRE],
            raw.at[i],
            ici_send,
            halo_recv,
            along(-a, -b),
            MESH,
        )
        halos[a, b].start()
    for a in (-2, 2):
        signal(token.at[0], along(a, 0))

    spacing = float(blocks * 128) ** (1.0 / 3.0) * math.sqrt(0.5)
    scale = jnp.ones((8, 128), F32)
    for k in range(3):
        scale = jnp.where(row8 == k, edge[k] * spacing, scale)
    scale = jnp.where(row8 == 6, 0.25 * lam, jnp.where(row8 == 7, lam, scale))
    base = jnp.where(row8 == 6, 0.15, 0.0)
    step_z = jnp.where(row8 == 2, scale, 0.0)
    lane32 = lax.broadcasted_iota(jnp.int32, (32, 128), 1).astype(F32)
    step_x = jnp.where(row8 == 0, jnp.where(lane8 < 16, 1.0, -1.0), 0.0)
    ones8 = jnp.ones((8, 128), BF16)
    ghost[27 * blocks] = jnp.where(row8 == 3, 1.0, jnp.where(row8 == 6, 0.15, 0.0))
    itself = []
    for q in range(blocks):
        times = jnp.int32(0)
        for e in range(listed):
            number = neighbours[0, 0, q, 0, e]
            domain = number // blocks
            where = (domain % 3) * plane + (domain // 3) * blocks + number % blocks
            where = jnp.where(e < counts[0, 0, 0, q], where, 3 * plane)
            places[q * listed + e] = where
            times += jnp.where(where == center + q, 1, 0)
        itself.append(jnp.full((1, 128), times, jnp.int32).astype(F32))
    around = ((0, 0), (0, 1), (0, -1), (-1, 0), (1, 0), (-1, 1), (1, 1), (-1, -1), (1, -1))
    pl.semaphore_wait(token.at[0], 2)
    for a in (-4, 4):
        signal(token.at[1], along(a, 0))
    wait_bytes(leavers.at[pl.ds(0, len(leaves))], leave_recv)

    for a, b in around:
        i = 3 * (a + 1) + b + 1
        here, above, below = (leavers[3 * (a + 2 + k) + b + 1] for k in (0, 1, -1))
        slots = jnp.broadcast_to(here.T[0:32, 7:8], (32, 128))
        tile = jnp.where(lane8 < 16, above, below) + step_x
        tile = jnp.where(row8 == 7, pltpu.roll(tile, 1, 0), tile)
        parts = jnp.concatenate((*split3(tile), ones8), axis=0)
        spread = jnp.concatenate(
            [
                (slots == lane32 + float(q * 128)).astype(F32).astype(BF16)
                for q in range(blocks)
            ],
            axis=1,
        )
        arrived = jnp.dot(parts[:, 0:32], spread, preferred_element_type=F32)
        rows_new = join3(arrived)
        for q in range(blocks):
            landed[i, q, 0:8] = rows_new[:, q * 128 : q * 128 + 128]
            landed[i, q, 8:16] = arrived[24:32, q * 128 : q * 128 + 128]

    wait_bytes(raw.at[pl.ds(0, len(halos))], halo_recv)
    for a, b in around:
        i = 3 * (a + 1) + b + 1
        offset = base
        for k, value in enumerate((a, b)):
            if value:
                offset = jnp.where(row8 == k, scale * float(value), offset)
        for q in range(blocks):
            moved = jnp.where(landed[i, q, 8:16] > 0.5, landed[i, q, 0:8], raw[i, q])
            ghost[plane + i * blocks + q] = moved * scale + offset
    pltpu.make_async_remote_copy(
        ghost.at[pl.ds(plane, plane)], theirs, ici_send, over_recv, along(0, 0, 1), MESH
    ).start()
    self_sums = [jnp.zeros((1, 128), F32)] * 3
    for q in range(blocks):
        tile = ghost[center + q]
        columns = tile.T
        for k in range(8):
            own[k, q * 128 : q * 128 + 128, :] = jnp.broadcast_to(
                columns[:, k : k + 1], (128, 128)
            )
        atom = [tile[r : r + 1] for r in range(8)]
        _, _, _, _, u, root, t, ty, coul = pair(atom, atom)
        v = (ty - t) + coul
        g = u * ty + 0.25 * (coul * (root * root))
        off = atom[7]
        self_sums = [
            total + itself[q] * term for total, term in zip(self_sums, (v, off * v, off * g))
        ]

    wait_bytes(theirs, over_recv)
    for i in range(plane):
        tile = theirs[i]
        ghost[i] = tile - step_z
        ghost[2 * plane + i] = tile + step_z

    steps = blocks * 128 // CHUNK

    def pair_step(with_energy, with_force, chunk=CHUNK):
        halves = chunk // 8

        def step(k, sums):
            q = k // (128 // chunk)
            atoms = [
                [own[r, pl.ds(k * chunk + 8 * half, 8), :] for r in range(8)]
                for half in range(halves)
            ]
            force = [[jnp.zeros((8, 128), F32)] * 3 for _ in atoms]
            for e in range(listed):
                place = places[q * listed + e]
                other = [ghost[place, r : r + 1, :] for r in range(8)]
                for half, atom in enumerate(atoms):
                    d, _, r4, inverse, u, root, t, ty, coul = pair(atom, other)
                    off = jnp.maximum(atom[7], other[7])
                    m = coul * (root * root)
                    if with_energy:
                        v_sum, ov_sum, og_sum = sums
                        v = (ty - t) + coul
                        g = u * ty + 0.25 * m
                        sums = v_sum + v, ov_sum + off * v, og_sum + off * g
                    if with_force:
                        f = ((r4 * inverse) * ty + m * (1.0 / 12.0)) * (1.0 - off)
                        force[half] = [total + f * part for total, part in zip(force[half], d)]
            if with_force:
                for half, totals in enumerate(force):
                    for axis, total in enumerate(totals):
                        force_acc[axis, pl.ds(k * chunk + 8 * half, 8), :] = total
            return sums

        return step

    zero = jnp.zeros((8, 128), F32)
    both = steps - LATE_A - LATE_B
    sums = lax.fori_loop(0, both, pair_step(True, True), (zero, zero, zero))
    pl.semaphore_wait(token.at[1], 2)
    for a in (-8, 8):
        signal(token.at[2], along(a, 0))
    wide = WIDE // CHUNK
    sums = lax.fori_loop(both // wide, steps // wide, pair_step(True, False, WIDE), sums)
    v_row, ov_row, og_row = (
        jnp.sum(total, axis=0, keepdims=True) - itself for total, itself in zip(sums, self_sums)
    )
    lane1 = lax.broadcasted_iota(jnp.int32, (1, 128), 1)
    energy_row = v_row - ov_row
    dhdl_row = ov_row + (0.5 * (1.0 - lam)) * og_row
    energy_row += pltpu.roll(energy_row, 64, 1)
    dhdl_row += pltpu.roll(dhdl_row, 64, 1)
    part = jnp.where(lane1 < 64, energy_row, dhdl_row)

    leader = me_z == n_dz - 1
    my_peer = me_y * n_dz + me_z
    plane_sums[my_peer] = part

    def send_part(b, c):
        pltpu.make_async_remote_copy(
            plane_sums.at[my_peer],
            plane_sums.at[my_peer],
            plane_send,
            plane_recv,
            along(0, b, c),
            MESH,
        ).start()

    @pl.when(jnp.logical_not(leader))
    def _():
        for b in (0, 1, -1, 2):
            send_part(b, 1)

    @pl.when(leader)
    def _():
        for b in (1, -1, 2):
            send_part(b, 0)

    lax.fori_loop(both, both + LATE_A, pair_step(False, True), ())
    ones = jnp.ones((8, 384), BF16)

    def row_sums(axis):
        for q in range(blocks):
            parts = jnp.concatenate(
                split3(force_acc[axis, q * 128 : q * 128 + 128, :]), axis=1
            )
            total = lax.dot_general(
                ones, parts, (((1,), (1,)), ((), ())), preferred_element_type=F32
            )
            forces_out[axis, 0, 0, :, q * 128 : q * 128 + 128] = total[0:1] * FORCE_SCALE

    @pl.when(leader)
    def _():
        wait_bytes(plane_sums.at[pl.ds(0, len(peers))], plane_recv)
        total = plane_sums[0]
        for i in range(1, n_dy * n_dz):
            total = total + plane_sums[i]
        line_sums[me_x] = total
        pl.semaphore_wait(token.at[2], 2)
        for d in sorted(range(1, n_dx), key=lambda d: min(d, n_dx - d)):
            pltpu.make_async_remote_copy(
                line_sums.at[me_x],
                line_sums.at[me_x],
                line_send,
                line_recv,
                along(d, 0),
                MESH,
            ).start()

    @pl.when(jnp.logical_not(leader))
    def _():
        pl.semaphore_wait(token.at[2], 2)

    lax.fori_loop(both + LATE_A, steps, pair_step(False, True), ())
    for axis in range(3):
        row_sums(axis)
    @pl.when(leader)
    def _():
        wait_bytes(line_sums.at[pl.ds(0, n_dx - 1)], line_recv)
        total = line_sums[0]
        for i in range(1, n_dx):
            total = total + line_sums[i]
        total_out[...] = total
        pltpu.make_async_remote_copy(
            total_out, total_in, total_send, total_recv, along(0, 0, 1), MESH
        ).start()

    @pl.when(jnp.logical_not(leader))
    def _():
        wait_bytes(total_in, total_recv)
        total_out[...] = total_in[...]

    total = total_out[...]
    norm = 0.5 / (blocks * 128 * n_dx * n_dy * n_dz)
    energy_out[0] = jnp.sum(jnp.where(lane1 < 64, total, 0.0)) * norm
    dhdl_out[0] = jnp.sum(jnp.where(lane1 < 64, 0.0, total)) * (-norm / lam)
    results = [
        pltpu.make_async_copy(energy_out, energy_hbm, out_sem.at[0]),
        pltpu.make_async_copy(dhdl_out, dhdl_hbm, out_sem.at[1]),
    ]
    for copy in results:
        copy.start()
    wait_bytes(ghost.at[pl.ds(0, len(leaves) + (len(halos) + 9) * blocks)], ici_send)

    @pl.when(leader)
    def _():
        wait_bytes(plane_sums.at[pl.ds(0, n_dy - 1)], plane_send)
        wait_bytes(line_sums.at[pl.ds(0, n_dx - 1)], line_send)
        wait_bytes(total_out, total_send)

    @pl.when(jnp.logical_not(leader))
    def _():
        wait_bytes(plane_sums.at[pl.ds(0, n_dy)], plane_send)

    for copy in results:
        copy.wait()


def on_device(
    fraction,
    atom_type,
    perturbed,
    leaving,
    neighbours,
    counts,
    sigma_table,
    depth_table,
    charge_table,
    domain_edge,
    coupling,
):
    n_dx, n_dy, n_dz = (lax.axis_size(axis) for axis in ("dx", "dy", "dz"))
    atoms = fraction.shape[-1]
    blocks = atoms // 128
    sizes = (n_dx, n_dy, n_dz, blocks, neighbours.shape[-1])
    neighbours = neighbours.transpose(0, 1, 3, 2, 4)
    hbm = pl.BlockSpec(memory_space=pltpu.HBM)
    dma, regular = pltpu.SemaphoreType.DMA, pltpu.SemaphoreType.REGULAR
    scalars = (
        leaving,
        neighbours,
        counts,
        sigma_table,
        depth_table,
        charge_table,
        domain_edge,
        coupling,
    )
    return pl.pallas_call(
        lambda *refs: kernel(sizes, *refs),
        out_shape=(
            pltpu.VMEM(fraction.shape, F32),
            jax.ShapeDtypeStruct((1,), F32),
            jax.ShapeDtypeStruct((1,), F32),
        ),
        in_specs=[hbm] * 11,
        out_specs=(pl.BlockSpec(memory_space=pltpu.VMEM), hbm, hbm),
        scratch_shapes=[
            pltpu.SMEM((1,), F32),
            pltpu.SMEM((1,), F32),
            *[pltpu.SMEM(array.shape, array.dtype) for array in scalars],
            pltpu.VMEM((2 * blocks, 128), jnp.int32),
            pltpu.VMEM((5 * blocks, 128), F32),
            pltpu.VMEM((4, blocks, 128), F32),
            pltpu.VMEM((9, blocks, 8, 128), F32),
            pltpu.VMEM((15, 8, 128), F32),
            pltpu.VMEM((9, blocks, 16, 128), F32),
            pltpu.VMEM((9 * blocks, 8, 128), F32),
            pltpu.VMEM((27 * blocks + 1, 8, 128), F32),
            pltpu.SMEM((blocks * neighbours.shape[-1],), jnp.int32),
            pltpu.VMEM((8, atoms, 128), F32),
            pltpu.VMEM((3, atoms, 128), F32),
            pltpu.VMEM((n_dy * n_dz, 1, 128), F32),
            pltpu.VMEM((n_dx, 1, 128), F32),
            pltpu.VMEM((1, 128), F32),
            pltpu.VMEM((1, 128), F32),
            dma((len(scalars),)),
            *[dma] * 11,
            dma((2,)),
            regular((3,)),
        ],
        compiler_params=pltpu.CompilerParams(
            collective_id=0, has_side_effects=True, vmem_limit_bytes=62 * 1024 * 1024
        ),
        name="step",
    )(
        fraction,
        atom_type,
        perturbed,
        leaving,
        neighbours,
        counts,
        sigma_table,
        depth_table,
        charge_table,
        domain_edge,
        coupling,
    )


def solution(mesh):
    return jax.shard_map(
        on_device,
        mesh=mesh,
        in_specs=(
            P(None, ("win", "dx"), "dy", "dz", None),
            P(("win", "dx"), "dy", "dz", None),
            P(("win", "dx"), "dy", "dz", None),
            P(("win", "dx"), "dy", "dz", None, None),
            P(("win", "dx"), "dy", "dz", None, None),
            P(("win", "dx"), "dy", "dz", None),
            P(),
            P(),
            P(),
            P(),
            P("win"),
        ),
        out_specs=(P(None, ("win", "dx"), "dy", "dz", None), P("win"), P("win")),
        check_vma=False,
    )
```

```python
import math

import jax
import jax.numpy as jnp
from jax import lax
from jax.experimental import pallas as pl
from jax.experimental.pallas import tpu as pltpu
from jax.sharding import PartitionSpec as P

F32 = jnp.float32
BF16 = jnp.bfloat16
MESH = pl.DeviceIdType.MESH

SIGMA_SCALE = 0.5 * 4.0 ** (-1.0 / 6.0)
CHARGE_SCALE = math.sqrt(0.1 / math.sqrt(2.0))
FORCE_SCALE = 12.0 * math.sqrt(0.5)
CENTRE = 4
LEAVE_CENTRE = 7
CHUNK = 16
WIDE = 32
LATE_A, LATE_B = 18, 18


def split3(x):
    high = x.astype(BF16)
    rest = x - high.astype(F32)
    mid = rest.astype(BF16)
    low = (rest - mid.astype(F32)).astype(BF16)
    return high, mid, low


def join3(x):
    return x[0:8] + (x[8:16] + x[16:24])


def pair(own, other):
    dx, dy, dz = own[0] - other[0], own[1] - other[1], own[2] - other[2]
    r2 = dx * dx + dy * dy + dz * dz
    c = jnp.maximum(own[6], other[6])
    h = own[3] + other[3]
    h2 = h * h
    s = h2 * h2 * h2
    r4 = r2 * r2
    inverse = 1.0 / (s * c + r4 * r2)
    u = s * inverse
    root = lax.rsqrt(c + r2)
    t = (own[4] * other[4]) * u
    ty = t * (u - 1.0)
    coul = (own[5] * other[5]) * root
    return (dx, dy, dz), c, r4, inverse, u, root, t, ty, coul


def kernel(
    sizes,
    frac_hbm,
    type_hbm,
    pert_hbm,
    leaving_hbm,
    neighbours_hbm,
    counts_hbm,
    sigma_hbm,
    depth_hbm,
    charge_hbm,
    edge_hbm,
    coupling_hbm,
    forces_out,
    energy_hbm,
    dhdl_hbm,
    energy_out,
    dhdl_out,
    leaving,
    neighbours,
    counts,
    sigma_table,
    depth_table,
    charge_table,
    edge,
    coupling,
    kinds,
    rows_in,
    table,
    raw,
    leavers,
    came,
    landed,
    theirs,
    ghost,
    places,
    own,
    force_acc,
    plane_sums,
    line_sums,
    total_out,
    total_in,
    in_sem,
    rows_sem,
    ici_send,
    leave_send,
    leave_recv,
    halo_recv,
    over_recv,
    plane_send,
    plane_recv,
    line_send,
    line_recv,
    total_send,
    total_recv,
    out_sem,
    token,
):
    n_dx, n_dy, n_dz, blocks, listed = sizes
    me_x, me_y, me_z = lax.axis_index("dx"), lax.axis_index("dy"), lax.axis_index("dz")

    def along(a, b, c=0):
        return {
            "dx": lax.rem(me_x + a % n_dx, n_dx),
            "dy": lax.rem(me_y + b % n_dy, n_dy),
            "dz": lax.rem(me_z + c, n_dz),
        }

    def signal(semaphore, device):
        pl.semaphore_signal(semaphore, inc=1, device_id=device, device_id_type=MESH)

    copies = [
        (leaving_hbm, leaving),
        (sigma_hbm, sigma_table),
        (depth_hbm, depth_table),
        (charge_hbm, charge_table),
        (coupling_hbm, coupling),
        (edge_hbm, edge),
        (neighbours_hbm, neighbours),
        (counts_hbm, counts),
    ]
    copies = [
        pltpu.make_async_copy(src, dst, in_sem.at[i]) for i, (src, dst) in enumerate(copies)
    ]
    for copy in copies:
        copy.start()
    for q in range(blocks):
        lanes = pl.ds(q * 128, 128)
        row_copies = [(frac_hbm.at[k, 0, 0, 0, lanes], raw.at[CENTRE, q, k]) for k in range(3)]
        row_copies.append((type_hbm.at[0, 0, 0, lanes], kinds.at[q]))
        row_copies.append((pert_hbm.at[0, 0, 0, lanes], kinds.at[blocks + q]))
        for src, dst in row_copies:
            pltpu.make_async_copy(src, dst, rows_sem).start()

    def wait_bytes(ref, semaphore):
        pltpu.make_async_copy(ref, ref, semaphore).wait()

    peers = [(b, c) for b in range(n_dy) for c in range(n_dz) if (b, c) != (0, 0)]
    near = [(a, b, 0) for a in (2, -2, 1, -1) for b in (1, -1, 0)]
    near += [(0, b, c) for b, c in peers]
    barrier = pltpu.get_barrier_semaphore()
    for device in near:
        signal(barrier, along(*device))

    row8 = lax.broadcasted_iota(jnp.int32, (8, 128), 0)
    lane8 = lax.broadcasted_iota(jnp.int32, (8, 128), 1)
    for copy in copies:
        copy.wait()
    wait_bytes(rows_in.at[pl.ds(0, 5 * blocks)], rows_sem)
    lam = coupling[0]
    plane = 9 * blocks
    center = plane + CENTRE * blocks

    lane32 = jnp.bitwise_and(lane8, 31)
    leave_slots = jnp.zeros((8, 128), jnp.int32)
    land_slots = jnp.zeros((8, 128), jnp.int32)
    for m in range(16):
        up, down = leaving[0, 0, 0, 0, m], leaving[0, 0, 0, 1, m]
        leave_slots = jnp.where(lane32 == m, down, jnp.where(lane32 == m + 16, up, leave_slots))
        land_slots = jnp.where(lane32 == m, up, jnp.where(lane32 == m + 16, down, land_slots))
    kind = kinds[0:blocks, :]
    sigma = jnp.zeros((blocks, 128), F32)
    depth = jnp.zeros((blocks, 128), F32)
    charge = jnp.zeros((blocks, 128), F32)
    for k in range(sigma_table.shape[0]):
        hit = kind == k
        sigma = jnp.where(hit, sigma_table[k], sigma)
        depth = jnp.where(hit, depth_table[k], depth)
        charge = jnp.where(hit, charge_table[k], charge)
    flag = kinds[blocks : 2 * blocks, :].astype(F32)
    table[0] = sigma * SIGMA_SCALE
    table[1] = jnp.sqrt(depth)
    table[2] = charge * CHARGE_SCALE
    table[3] = flag
    for q in range(blocks):
        for k in range(5):
            raw[CENTRE, q, 3 + k : 4 + k, :] = table[min(k, 3), q : q + 1, :]

    rows = lax.broadcasted_iota(jnp.int32, (128, 128), 0)
    gathered = jnp.zeros((24, 128), F32)
    for q in range(blocks):
        pick = (leave_slots[0:1] == rows + q * 128).astype(F32).astype(BF16)
        parts = jnp.concatenate(split3(raw[CENTRE, q]), axis=0)
        gathered += jnp.dot(parts, pick, preferred_element_type=F32)
    going = jnp.where(row8 == 7, land_slots.astype(F32), join3(gathered))
    quarter = lax.broadcasted_iota(jnp.int32, (1, 128), 1) // 32
    for half in range(2):
        line = going[4 * half : 4 * half + 1]
        for k in range(1, 4):
            line = jnp.where(quarter == k, going[4 * half + k : 4 * half + k + 1], line)
        leavers[LEAVE_CENTRE, half : half + 1, :] = line

    pl.semaphore_wait(barrier, len(near))
    leaves, halos = {}, {}
    for a in (2, -2, 1, -1, 0):
        for b in (1, -1, 0):
            if (a, b) != (0, 0):
                i = 3 * (a + 2) + b + 1
                leaves[a, b] = pltpu.make_async_remote_copy(
                    leavers.at[LEAVE_CENTRE],
                    leavers.at[i],
                    leave_send,
                    leave_recv,
                    along(-a, -b),
                    MESH,
                )
                leaves[a, b].start()
    for a, b in ((-1, 0), (1, 0), (0, 1), (0, -1), (1, 1), (-1, 1), (1, -1), (-1, -1)):
        i = 3 * (a + 1) + b + 1
        halos[a, b] = pltpu.make_async_remote_copy(
            raw.at[CENTRE],
            raw.at[i],
            ici_send,
            halo_recv,
            along(-a, -b),
            MESH,
        )
        halos[a, b].start()
    for a in (-2, 2):
        signal(token.at[0], along(a, 0))

    spacing = float(blocks * 128) ** (1.0 / 3.0) * math.sqrt(0.5)
    scale = jnp.ones((8, 128), F32)
    for k in range(3):
        scale = jnp.where(row8 == k, edge[k] * spacing, scale)
    scale = jnp.where(row8 == 6, 0.25 * lam, jnp.where(row8 == 7, lam, scale))
    base = jnp.where(row8 == 6, 0.15, 0.0)
    step_z = jnp.where(row8 == 2, scale, 0.0)
    lane32 = lax.broadcasted_iota(jnp.int32, (32, 128), 1).astype(F32)
    step_x = jnp.where(row8 == 0, jnp.where(lane8 < 16, 1.0, -1.0), 0.0)
    ones8 = jnp.ones((8, 128), BF16)
    ghost[27 * blocks] = jnp.where(row8 == 3, 1.0, jnp.where(row8 == 6, 0.15, 0.0))
    itself = []
    for q in range(blocks):
        times = jnp.int32(0)
        for e in range(listed):
            number = neighbours[0, 0, q, 0, e]
            domain = number // blocks
            where = (domain % 3) * plane + (domain // 3) * blocks + number % blocks
            where = jnp.where(e < counts[0, 0, 0, q], where, 3 * plane)
            places[q * listed + e] = where
            times += jnp.where(where == center + q, 1, 0)
        itself.append(jnp.full((1, 128), times, jnp.int32).astype(F32))
    around = ((0, 0), (0, 1), (0, -1), (-1, 0), (1, 0), (-1, 1), (1, 1), (-1, -1), (1, -1))
    pl.semaphore_wait(token.at[0], 2)
    for a in (-4, 4):
        signal(token.at[1], along(a, 0))
    wait_bytes(leavers.at[pl.ds(0, len(leaves))], leave_recv)

    for i in range(15):
        packed = leavers[i]
        for k in range(4):
            lines = packed if k == 0 else pltpu.roll(packed, 128 - 32 * k, 1)
            for half in range(2):
                came[i, 4 * half + k : 4 * half + k + 1, :] = lines[half : half + 1]
    places_in = jnp.concatenate([came[3 + i, 7:8, :] for i in range(9)], axis=0).T
    for a, b in around:
        i = 3 * (a + 1) + b + 1
        above, below = (came[3 * (a + 2 + k) + b + 1] for k in (1, -1))
        slots = jnp.broadcast_to(places_in[0:32, i : i + 1], (32, 128))
        tile = jnp.where(lane8 < 16, above, below) + step_x
        tile = jnp.where(row8 == 7, pltpu.roll(tile, 1, 0), tile)
        parts = jnp.concatenate((*split3(tile), ones8), axis=0)
        spread = jnp.concatenate(
            [
                (slots == lane32 + float(q * 128)).astype(F32).astype(BF16)
                for q in range(blocks)
            ],
            axis=1,
        )
        arrived = jnp.dot(parts[:, 0:32], spread, preferred_element_type=F32)
        rows_new = join3(arrived)
        for q in range(blocks):
            landed[i, q, 0:8] = rows_new[:, q * 128 : q * 128 + 128]
            landed[i, q, 8:16] = arrived[24:32, q * 128 : q * 128 + 128]

    wait_bytes(raw.at[pl.ds(0, len(halos))], halo_recv)
    for a, b in around:
        i = 3 * (a + 1) + b + 1
        offset = base
        for k, value in enumerate((a, b)):
            if value:
                offset = jnp.where(row8 == k, scale * float(value), offset)
        for q in range(blocks):
            moved = jnp.where(landed[i, q, 8:16] > 0.5, landed[i, q, 0:8], raw[i, q])
            ghost[plane + i * blocks + q] = moved * scale + offset
    pltpu.make_async_remote_copy(
        ghost.at[pl.ds(plane, plane)], theirs, ici_send, over_recv, along(0, 0, 1), MESH
    ).start()
    self_sums = [jnp.zeros((1, 128), F32)] * 3
    columns = jnp.concatenate([ghost[center + q] for q in range(blocks)], axis=0).T
    for q in range(blocks):
        tile = ghost[center + q]
        for k in range(8):
            own[k, q * 128 : q * 128 + 128, :] = jnp.broadcast_to(
                columns[:, 8 * q + k : 8 * q + k + 1], (128, 128)
            )
        atom = [tile[r : r + 1] for r in range(8)]
        _, _, _, _, u, root, t, ty, coul = pair(atom, atom)
        v = (ty - t) + coul
        g = u * ty + 0.25 * (coul * (root * root))
        off = atom[7]
        self_sums = [
            total + itself[q] * term for total, term in zip(self_sums, (v, off * v, off * g))
        ]

    wait_bytes(theirs, over_recv)
    for i in range(plane):
        tile = theirs[i]
        ghost[i] = tile - step_z
        ghost[2 * plane + i] = tile + step_z

    steps = blocks * 128 // CHUNK

    def pair_step(with_energy, with_force, chunk=CHUNK):
        halves = chunk // 8

        def step(k, sums):
            q = k // (128 // chunk)
            atoms = [
                [own[r, pl.ds(k * chunk + 8 * half, 8), :] for r in range(8)]
                for half in range(halves)
            ]
            force = [[jnp.zeros((8, 128), F32)] * 3 for _ in atoms]
            for e in range(listed):
                place = places[q * listed + e]
                other = [ghost[place, r : r + 1, :] for r in range(8)]
                for half, atom in enumerate(atoms):
                    d, _, r4, inverse, u, root, t, ty, coul = pair(atom, other)
                    off = jnp.maximum(atom[7], other[7])
                    m = coul * (root * root)
                    if with_energy:
                        v_sum, ov_sum, og_sum = sums
                        v = (ty - t) + coul
                        g = u * ty + 0.25 * m
                        sums = v_sum + v, ov_sum + off * v, og_sum + off * g
                    if with_force:
                        f = ((r4 * inverse) * ty + m * (1.0 / 12.0)) * (1.0 - off)
                        force[half] = [total + f * part for total, part in zip(force[half], d)]
            if with_force:
                for half, totals in enumerate(force):
                    for axis, total in enumerate(totals):
                        force_acc[axis, pl.ds(k * chunk + 8 * half, 8), :] = total
            return sums

        return step

    zero = jnp.zeros((8, 128), F32)
    both = steps - LATE_A - LATE_B
    sums = lax.fori_loop(0, both, pair_step(True, True), (zero, zero, zero))
    pl.semaphore_wait(token.at[1], 2)
    for a in (-8, 8):
        signal(token.at[2], along(a, 0))
    wide = WIDE // CHUNK
    sums = lax.fori_loop(both // wide, steps // wide, pair_step(True, False, WIDE), sums)
    v_row, ov_row, og_row = (
        jnp.sum(total, axis=0, keepdims=True) - itself for total, itself in zip(sums, self_sums)
    )
    lane1 = lax.broadcasted_iota(jnp.int32, (1, 128), 1)
    energy_row = v_row - ov_row
    dhdl_row = ov_row + (0.5 * (1.0 - lam)) * og_row
    energy_row += pltpu.roll(energy_row, 64, 1)
    dhdl_row += pltpu.roll(dhdl_row, 64, 1)
    part = jnp.where(lane1 < 64, energy_row, dhdl_row)

    leader = me_z == n_dz - 1
    my_peer = me_y * n_dz + me_z
    plane_sums[my_peer] = part

    def send_part(b, c):
        pltpu.make_async_remote_copy(
            plane_sums.at[my_peer],
            plane_sums.at[my_peer],
            plane_send,
            plane_recv,
            along(0, b, c),
            MESH,
        ).start()

    @pl.when(jnp.logical_not(leader))
    def _():
        for b in (0, 1, -1, 2):
            send_part(b, 1)

    @pl.when(leader)
    def _():
        for b in (1, -1, 2):
            send_part(b, 0)

    lax.fori_loop(both, both + LATE_A, pair_step(False, True), ())
    ones = jnp.ones((8, 384), BF16)

    def row_sums(axis):
        for q in range(blocks):
            parts = jnp.concatenate(
                split3(force_acc[axis, q * 128 : q * 128 + 128, :]), axis=1
            )
            total = lax.dot_general(
                ones, parts, (((1,), (1,)), ((), ())), preferred_element_type=F32
            )
            forces_out[axis, 0, 0, :, q * 128 : q * 128 + 128] = total[0:1] * FORCE_SCALE

    @pl.when(leader)
    def _():
        wait_bytes(plane_sums.at[pl.ds(0, len(peers))], plane_recv)
        total = plane_sums[0]
        for i in range(1, n_dy * n_dz):
            total = total + plane_sums[i]
        line_sums[me_x] = total
        pl.semaphore_wait(token.at[2], 2)
        for d in sorted(range(1, n_dx), key=lambda d: min(d, n_dx - d)):
            pltpu.make_async_remote_copy(
                line_sums.at[me_x],
                line_sums.at[me_x],
                line_send,
                line_recv,
                along(d, 0),
                MESH,
            ).start()

    @pl.when(jnp.logical_not(leader))
    def _():
        pl.semaphore_wait(token.at[2], 2)

    lax.fori_loop(both + LATE_A, steps, pair_step(False, True), ())
    for axis in range(3):
        row_sums(axis)
    @pl.when(leader)
    def _():
        wait_bytes(line_sums.at[pl.ds(0, n_dx - 1)], line_recv)
        total = line_sums[0]
        for i in range(1, n_dx):
            total = total + line_sums[i]
        total_out[...] = total
        pltpu.make_async_remote_copy(
            total_out, total_in, total_send, total_recv, along(0, 0, 1), MESH
        ).start()

    @pl.when(jnp.logical_not(leader))
    def _():
        wait_bytes(total_in, total_recv)
        total_out[...] = total_in[...]

    total = total_out[...]
    norm = 0.5 / (blocks * 128 * n_dx * n_dy * n_dz)
    energy_out[0] = jnp.sum(jnp.where(lane1 < 64, total, 0.0)) * norm
    dhdl_out[0] = jnp.sum(jnp.where(lane1 < 64, 0.0, total)) * (-norm / lam)
    results = [
        pltpu.make_async_copy(energy_out, energy_hbm, out_sem.at[0]),
        pltpu.make_async_copy(dhdl_out, dhdl_hbm, out_sem.at[1]),
    ]
    for copy in results:
        copy.start()
    wait_bytes(leavers.at[pl.ds(0, len(leaves))], leave_send)
    wait_bytes(ghost.at[pl.ds(0, (len(halos) + 9) * blocks)], ici_send)

    @pl.when(leader)
    def _():
        wait_bytes(plane_sums.at[pl.ds(0, n_dy - 1)], plane_send)
        wait_bytes(line_sums.at[pl.ds(0, n_dx - 1)], line_send)
        wait_bytes(total_out, total_send)

    @pl.when(jnp.logical_not(leader))
    def _():
        wait_bytes(plane_sums.at[pl.ds(0, n_dy)], plane_send)

    for copy in results:
        copy.wait()


def on_device(
    fraction,
    atom_type,
    perturbed,
    leaving,
    neighbours,
    counts,
    sigma_table,
    depth_table,
    charge_table,
    domain_edge,
    coupling,
):
    n_dx, n_dy, n_dz = (lax.axis_size(axis) for axis in ("dx", "dy", "dz"))
    atoms = fraction.shape[-1]
    blocks = atoms // 128
    sizes = (n_dx, n_dy, n_dz, blocks, neighbours.shape[-1])
    neighbours = neighbours.transpose(0, 1, 3, 2, 4)
    hbm = pl.BlockSpec(memory_space=pltpu.HBM)
    dma, regular = pltpu.SemaphoreType.DMA, pltpu.SemaphoreType.REGULAR
    scalars = (
        leaving,
        neighbours,
        counts,
        sigma_table,
        depth_table,
        charge_table,
        domain_edge,
        coupling,
    )
    return pl.pallas_call(
        lambda *refs: kernel(sizes, *refs),
        out_shape=(
            pltpu.VMEM(fraction.shape, F32),
            jax.ShapeDtypeStruct((1,), F32),
            jax.ShapeDtypeStruct((1,), F32),
        ),
        in_specs=[hbm] * 11,
        out_specs=(pl.BlockSpec(memory_space=pltpu.VMEM), hbm, hbm),
        scratch_shapes=[
            pltpu.SMEM((1,), F32),
            pltpu.SMEM((1,), F32),
            *[pltpu.SMEM(array.shape, array.dtype) for array in scalars],
            pltpu.VMEM((2 * blocks, 128), jnp.int32),
            pltpu.VMEM((5 * blocks, 128), F32),
            pltpu.VMEM((4, blocks, 128), F32),
            pltpu.VMEM((9, blocks, 8, 128), F32),
            pltpu.VMEM((15, 2, 128), F32),
            pltpu.VMEM((15, 8, 128), F32),
            pltpu.VMEM((9, blocks, 16, 128), F32),
            pltpu.VMEM((9 * blocks, 8, 128), F32),
            pltpu.VMEM((27 * blocks + 1, 8, 128), F32),
            pltpu.SMEM((blocks * neighbours.shape[-1],), jnp.int32),
            pltpu.VMEM((8, atoms, 128), F32),
            pltpu.VMEM((3, atoms, 128), F32),
            pltpu.VMEM((n_dy * n_dz, 1, 128), F32),
            pltpu.VMEM((n_dx, 1, 128), F32),
            pltpu.VMEM((1, 128), F32),
            pltpu.VMEM((1, 128), F32),
            dma((len(scalars),)),
            *[dma] * 12,
            dma((2,)),
            regular((3,)),
        ],
        compiler_params=pltpu.CompilerParams(
            collective_id=0, has_side_effects=True, vmem_limit_bytes=62 * 1024 * 1024
        ),
        name="step",
    )(
        fraction,
        atom_type,
        perturbed,
        leaving,
        neighbours,
        counts,
        sigma_table,
        depth_table,
        charge_table,
        domain_edge,
        coupling,
    )


def solution(mesh):
    return jax.shard_map(
        on_device,
        mesh=mesh,
        in_specs=(
            P(None, ("win", "dx"), "dy", "dz", None),
            P(("win", "dx"), "dy", "dz", None),
            P(("win", "dx"), "dy", "dz", None),
            P(("win", "dx"), "dy", "dz", None, None),
            P(("win", "dx"), "dy", "dz", None, None),
            P(("win", "dx"), "dy", "dz", None),
            P(),
            P(),
            P(),
            P(),
            P("win"),
        ),
        out_specs=(P(None, ("win", "dx"), "dy", "dz", None), P("win"), P("win")),
        check_vma=False,
    )
```

```python
import math

import jax
import jax.numpy as jnp
from jax import lax
from jax.experimental import pallas as pl
from jax.experimental.pallas import tpu as pltpu
from jax.sharding import PartitionSpec as P

F32 = jnp.float32
BF16 = jnp.bfloat16
MESH = pl.DeviceIdType.MESH

SIGMA_SCALE = 0.5 * 4.0 ** (-1.0 / 6.0)
CHARGE_SCALE = math.sqrt(0.1 / math.sqrt(2.0))
FORCE_SCALE = 12.0 * math.sqrt(0.5)
CENTRE = 4
LEAVE_CENTRE = 7
CHUNK = 16
WIDE = 32
LATE_A, LATE_B = 18, 18


def split3(x):
    high = x.astype(BF16)
    rest = x - high.astype(F32)
    mid = rest.astype(BF16)
    low = (rest - mid.astype(F32)).astype(BF16)
    return high, mid, low


def join3(x):
    return x[0:8] + (x[8:16] + x[16:24])


def pair(own, other):
    dx, dy, dz = own[0] - other[0], own[1] - other[1], own[2] - other[2]
    r2 = dx * dx + dy * dy + dz * dz
    c = jnp.maximum(own[6], other[6])
    h = own[3] + other[3]
    h2 = h * h
    s = h2 * h2 * h2
    r4 = r2 * r2
    inverse = 1.0 / (s * c + r4 * r2)
    u = s * inverse
    root = lax.rsqrt(c + r2)
    t = (own[4] * other[4]) * u
    ty = t * (u - 1.0)
    coul = (own[5] * other[5]) * root
    return (dx, dy, dz), c, r4, inverse, u, root, t, ty, coul


def kernel(
    sizes,
    frac_hbm,
    type_hbm,
    pert_hbm,
    leaving_hbm,
    neighbours_hbm,
    counts_hbm,
    sigma_hbm,
    depth_hbm,
    charge_hbm,
    edge_hbm,
    coupling_hbm,
    forces_out,
    energy_hbm,
    dhdl_hbm,
    energy_out,
    dhdl_out,
    leaving,
    neighbours,
    counts,
    sigma_table,
    depth_table,
    charge_table,
    edge,
    coupling,
    kinds,
    rows_in,
    table,
    raw,
    leavers,
    came,
    landed,
    theirs,
    ghost,
    places,
    columns,
    own,
    force_acc,
    plane_sums,
    line_sums,
    total_out,
    total_in,
    in_sem,
    rows_sem,
    ici_send,
    leave_send,
    leave_recv,
    halo_recv,
    over_recv,
    plane_send,
    plane_recv,
    line_send,
    line_recv,
    total_send,
    total_recv,
    out_sem,
    token,
):
    n_dx, n_dy, n_dz, blocks, listed = sizes
    me_x, me_y, me_z = lax.axis_index("dx"), lax.axis_index("dy"), lax.axis_index("dz")

    def along(a, b, c=0):
        return {
            "dx": lax.rem(me_x + a % n_dx, n_dx),
            "dy": lax.rem(me_y + b % n_dy, n_dy),
            "dz": lax.rem(me_z + c, n_dz),
        }

    def signal(semaphore, device):
        pl.semaphore_signal(semaphore, inc=1, device_id=device, device_id_type=MESH)

    copies = [
        (leaving_hbm, leaving),
        (sigma_hbm, sigma_table),
        (depth_hbm, depth_table),
        (charge_hbm, charge_table),
        (coupling_hbm, coupling),
        (edge_hbm, edge),
        (neighbours_hbm, neighbours),
        (counts_hbm, counts),
    ]
    copies = [
        pltpu.make_async_copy(src, dst, in_sem.at[i]) for i, (src, dst) in enumerate(copies)
    ]
    for copy in copies:
        copy.start()
    for q in range(blocks):
        lanes = pl.ds(q * 128, 128)
        row_copies = [(frac_hbm.at[k, 0, 0, 0, lanes], raw.at[CENTRE, q, k]) for k in range(3)]
        row_copies.append((type_hbm.at[0, 0, 0, lanes], kinds.at[q]))
        row_copies.append((pert_hbm.at[0, 0, 0, lanes], kinds.at[blocks + q]))
        for src, dst in row_copies:
            pltpu.make_async_copy(src, dst, rows_sem).start()

    def wait_bytes(ref, semaphore):
        pltpu.make_async_copy(ref, ref, semaphore).wait()

    peers = [(b, c) for b in range(n_dy) for c in range(n_dz) if (b, c) != (0, 0)]
    near = [(a, b, 0) for a in (2, -2, 1, -1) for b in (1, -1, 0)]
    near += [(0, b, c) for b, c in peers]
    barrier = pltpu.get_barrier_semaphore()
    for device in near:
        signal(barrier, along(*device))

    row8 = lax.broadcasted_iota(jnp.int32, (8, 128), 0)
    lane8 = lax.broadcasted_iota(jnp.int32, (8, 128), 1)
    for copy in copies:
        copy.wait()
    wait_bytes(rows_in.at[pl.ds(0, 5 * blocks)], rows_sem)
    lam = coupling[0]
    plane = 9 * blocks
    center = plane + CENTRE * blocks

    lane32 = jnp.bitwise_and(lane8, 31)
    leave_slots = jnp.zeros((8, 128), jnp.int32)
    land_slots = jnp.zeros((8, 128), jnp.int32)
    for m in range(16):
        up, down = leaving[0, 0, 0, 0, m], leaving[0, 0, 0, 1, m]
        leave_slots = jnp.where(lane32 == m, down, jnp.where(lane32 == m + 16, up, leave_slots))
        land_slots = jnp.where(lane32 == m, up, jnp.where(lane32 == m + 16, down, land_slots))
    kind = kinds[0:blocks, :]
    sigma = jnp.zeros((blocks, 128), F32)
    depth = jnp.zeros((blocks, 128), F32)
    charge = jnp.zeros((blocks, 128), F32)
    for k in range(sigma_table.shape[0]):
        hit = kind == k
        sigma = jnp.where(hit, sigma_table[k], sigma)
        depth = jnp.where(hit, depth_table[k], depth)
        charge = jnp.where(hit, charge_table[k], charge)
    flag = kinds[blocks : 2 * blocks, :].astype(F32)
    table[0] = sigma * SIGMA_SCALE
    table[1] = jnp.sqrt(depth)
    table[2] = charge * CHARGE_SCALE
    table[3] = flag
    for q in range(blocks):
        for k in range(5):
            raw[CENTRE, q, 3 + k : 4 + k, :] = table[min(k, 3), q : q + 1, :]

    rows = lax.broadcasted_iota(jnp.int32, (128, 128), 0)
    gathered = jnp.zeros((24, 128), F32)
    for q in range(blocks):
        pick = (leave_slots[0:1] == rows + q * 128).astype(F32).astype(BF16)
        parts = jnp.concatenate(split3(raw[CENTRE, q]), axis=0)
        gathered += jnp.dot(parts, pick, preferred_element_type=F32)
    going = jnp.where(row8 == 7, land_slots.astype(F32), join3(gathered))
    quarter = lax.broadcasted_iota(jnp.int32, (1, 128), 1) // 32
    for half in range(2):
        line = going[4 * half : 4 * half + 1]
        for k in range(1, 4):
            line = jnp.where(quarter == k, going[4 * half + k : 4 * half + k + 1], line)
        leavers[LEAVE_CENTRE, half : half + 1, :] = line

    pl.semaphore_wait(barrier, len(near))
    leaves, halos = {}, {}
    for a in (2, -2, 1, -1, 0):
        for b in (1, -1, 0):
            if (a, b) != (0, 0):
                i = 3 * (a + 2) + b + 1
                leaves[a, b] = pltpu.make_async_remote_copy(
                    leavers.at[LEAVE_CENTRE],
                    leavers.at[i],
                    leave_send,
                    leave_recv,
                    along(-a, -b),
                    MESH,
                )
                leaves[a, b].start()
    for a, b in ((-1, 0), (1, 0), (0, 1), (0, -1), (1, 1), (-1, 1), (1, -1), (-1, -1)):
        i = 3 * (a + 1) + b + 1
        halos[a, b] = pltpu.make_async_remote_copy(
            raw.at[CENTRE],
            raw.at[i],
            ici_send,
            halo_recv,
            along(-a, -b),
            MESH,
        )
        halos[a, b].start()
    for a in (-2, 2):
        signal(token.at[0], along(a, 0))

    spacing = float(blocks * 128) ** (1.0 / 3.0) * math.sqrt(0.5)
    scale = jnp.ones((8, 128), F32)
    for k in range(3):
        scale = jnp.where(row8 == k, edge[k] * spacing, scale)
    scale = jnp.where(row8 == 6, 0.25 * lam, jnp.where(row8 == 7, lam, scale))
    base = jnp.where(row8 == 6, 0.15, 0.0)
    step_z = jnp.where(row8 == 2, scale, 0.0)
    lane32 = lax.broadcasted_iota(jnp.int32, (32, 128), 1).astype(F32)
    step_x = jnp.where(row8 == 0, jnp.where(lane8 < 16, 1.0, -1.0), 0.0)
    ones8 = jnp.ones((8, 128), BF16)
    ghost[27 * blocks] = jnp.where(row8 == 3, 1.0, jnp.where(row8 == 6, 0.15, 0.0))
    itself = []
    for q in range(blocks):
        times = jnp.int32(0)
        for e in range(listed):
            number = neighbours[0, 0, q, 0, e]
            domain = number // blocks
            where = (domain % 3) * plane + (domain // 3) * blocks + number % blocks
            where = jnp.where(e < counts[0, 0, 0, q], where, 3 * plane)
            places[q * listed + e] = where
            times += jnp.where(where == center + q, 1, 0)
        itself.append(jnp.full((1, 128), times, jnp.int32).astype(F32))
    around = ((0, 0), (0, 1), (0, -1), (-1, 0), (1, 0), (-1, 1), (1, 1), (-1, -1), (1, -1))
    pl.semaphore_wait(token.at[0], 2)
    for a in (-4, 4):
        signal(token.at[1], along(a, 0))
    wait_bytes(leavers.at[pl.ds(0, len(leaves))], leave_recv)

    for i in range(15):
        packed = leavers[i]
        for k in range(4):
            lines = packed if k == 0 else pltpu.roll(packed, 128 - 32 * k, 1)
            for half in range(2):
                came[i, 4 * half + k : 4 * half + k + 1, :] = lines[half : half + 1]
    places_in = jnp.concatenate([came[3 + i, 7:8, :] for i in range(9)], axis=0).T
    for a, b in around:
        i = 3 * (a + 1) + b + 1
        above, below = (came[3 * (a + 2 + k) + b + 1] for k in (1, -1))
        slots = jnp.broadcast_to(places_in[0:32, i : i + 1], (32, 128))
        tile = jnp.where(lane8 < 16, above, below) + step_x
        tile = jnp.where(row8 == 7, pltpu.roll(tile, 1, 0), tile)
        parts = jnp.concatenate((*split3(tile), ones8), axis=0)
        spread = jnp.concatenate(
            [
                (slots == lane32 + float(q * 128)).astype(F32).astype(BF16)
                for q in range(blocks)
            ],
            axis=1,
        )
        arrived = jnp.dot(parts[:, 0:32], spread, preferred_element_type=F32)
        rows_new = join3(arrived)
        for q in range(blocks):
            landed[i, q, 0:8] = rows_new[:, q * 128 : q * 128 + 128]
            landed[i, q, 8:16] = arrived[24:32, q * 128 : q * 128 + 128]

    wait_bytes(raw.at[pl.ds(0, len(halos))], halo_recv)
    for a, b in around:
        i = 3 * (a + 1) + b + 1
        offset = base
        for k, value in enumerate((a, b)):
            if value:
                offset = jnp.where(row8 == k, scale * float(value), offset)
        for q in range(blocks):
            moved = jnp.where(landed[i, q, 8:16] > 0.5, landed[i, q, 0:8], raw[i, q])
            ghost[plane + i * blocks + q] = moved * scale + offset
    pltpu.make_async_remote_copy(
        ghost.at[pl.ds(plane, plane)], theirs, ici_send, over_recv, along(0, 0, 1), MESH
    ).start()
    self_sums = [jnp.zeros((1, 128), F32)] * 3
    def spread_own(first, atoms):
        for at in range(0, atoms, 8):
            spot = pl.multiple_of(first + at, 8)
            column = columns[pl.ds(spot, 8), :]
            for k in range(8):
                own[k, pl.ds(spot, 8), :] = jnp.broadcast_to(column[:, k : k + 1], (8, 128))

    for q in range(blocks):
        columns[q * 128 : q * 128 + 128, :] = ghost[center + q].T
    spread_own(0, CHUNK)
    for q in range(blocks):
        tile = ghost[center + q]
        atom = [tile[r : r + 1] for r in range(8)]
        _, _, _, _, u, root, t, ty, coul = pair(atom, atom)
        v = (ty - t) + coul
        g = u * ty + 0.25 * (coul * (root * root))
        off = atom[7]
        self_sums = [
            total + itself[q] * term for total, term in zip(self_sums, (v, off * v, off * g))
        ]

    wait_bytes(theirs, over_recv)
    for i in range(plane):
        tile = theirs[i]
        ghost[i] = tile - step_z
        ghost[2 * plane + i] = tile + step_z

    steps = blocks * 128 // CHUNK

    def pair_step(with_energy, with_force, chunk=CHUNK):
        halves = chunk // 8

        def step(k, sums):
            q = k // (128 // chunk)
            if with_energy:
                spread_own(jnp.minimum((k + 1) * chunk, blocks * 128 - WIDE), WIDE)
            atoms = [
                [own[r, pl.ds(k * chunk + 8 * half, 8), :] for r in range(8)]
                for half in range(halves)
            ]
            force = [[jnp.zeros((8, 128), F32)] * 3 for _ in atoms]
            for e in range(listed):
                place = places[q * listed + e]
                other = [ghost[place, r : r + 1, :] for r in range(8)]
                for half, atom in enumerate(atoms):
                    d, _, r4, inverse, u, root, t, ty, coul = pair(atom, other)
                    off = jnp.maximum(atom[7], other[7])
                    m = coul * (root * root)
                    if with_energy:
                        v_sum, ov_sum, og_sum = sums
                        v = (ty - t) + coul
                        g = u * ty + 0.25 * m
                        sums = v_sum + v, ov_sum + off * v, og_sum + off * g
                    if with_force:
                        f = ((r4 * inverse) * ty + m * (1.0 / 12.0)) * (1.0 - off)
                        force[half] = [total + f * part for total, part in zip(force[half], d)]
            if with_force:
                for half, totals in enumerate(force):
                    for axis, total in enumerate(totals):
                        force_acc[axis, pl.ds(k * chunk + 8 * half, 8), :] = total
            return sums

        return step

    zero = jnp.zeros((8, 128), F32)
    both = steps - LATE_A - LATE_B
    sums = lax.fori_loop(0, both, pair_step(True, True), (zero, zero, zero))
    pl.semaphore_wait(token.at[1], 2)
    for a in (-8, 8):
        signal(token.at[2], along(a, 0))
    wide = WIDE // CHUNK
    sums = lax.fori_loop(both // wide, steps // wide, pair_step(True, False, WIDE), sums)
    v_row, ov_row, og_row = (
        jnp.sum(total, axis=0, keepdims=True) - itself for total, itself in zip(sums, self_sums)
    )
    lane1 = lax.broadcasted_iota(jnp.int32, (1, 128), 1)
    energy_row = v_row - ov_row
    dhdl_row = ov_row + (0.5 * (1.0 - lam)) * og_row
    energy_row += pltpu.roll(energy_row, 64, 1)
    dhdl_row += pltpu.roll(dhdl_row, 64, 1)
    part = jnp.where(lane1 < 64, energy_row, dhdl_row)

    leader = me_z == n_dz - 1
    my_peer = me_y * n_dz + me_z
    plane_sums[my_peer] = part

    def send_part(b, c):
        pltpu.make_async_remote_copy(
            plane_sums.at[my_peer],
            plane_sums.at[my_peer],
            plane_send,
            plane_recv,
            along(0, b, c),
            MESH,
        ).start()

    @pl.when(jnp.logical_not(leader))
    def _():
        for b in (0, 1, -1, 2):
            send_part(b, 1)

    @pl.when(leader)
    def _():
        for b in (1, -1, 2):
            send_part(b, 0)

    lax.fori_loop(both, both + LATE_A, pair_step(False, True), ())
    ones = jnp.ones((8, 384), BF16)

    def row_sums(axis):
        for q in range(blocks):
            parts = jnp.concatenate(
                split3(force_acc[axis, q * 128 : q * 128 + 128, :]), axis=1
            )
            total = lax.dot_general(
                ones, parts, (((1,), (1,)), ((), ())), preferred_element_type=F32
            )
            forces_out[axis, 0, 0, :, q * 128 : q * 128 + 128] = total[0:1] * FORCE_SCALE

    @pl.when(leader)
    def _():
        wait_bytes(plane_sums.at[pl.ds(0, len(peers))], plane_recv)
        total = plane_sums[0]
        for i in range(1, n_dy * n_dz):
            total = total + plane_sums[i]
        line_sums[me_x] = total
        pl.semaphore_wait(token.at[2], 2)
        for d in sorted(range(1, n_dx), key=lambda d: min(d, n_dx - d)):
            pltpu.make_async_remote_copy(
                line_sums.at[me_x],
                line_sums.at[me_x],
                line_send,
                line_recv,
                along(d, 0),
                MESH,
            ).start()

    @pl.when(jnp.logical_not(leader))
    def _():
        pl.semaphore_wait(token.at[2], 2)

    lax.fori_loop(both + LATE_A, steps, pair_step(False, True), ())
    for axis in range(3):
        row_sums(axis)
    @pl.when(leader)
    def _():
        wait_bytes(line_sums.at[pl.ds(0, n_dx - 1)], line_recv)
        total = line_sums[0]
        for i in range(1, n_dx):
            total = total + line_sums[i]
        total_out[...] = total
        pltpu.make_async_remote_copy(
            total_out, total_in, total_send, total_recv, along(0, 0, 1), MESH
        ).start()

    @pl.when(jnp.logical_not(leader))
    def _():
        wait_bytes(total_in, total_recv)
        total_out[...] = total_in[...]

    total = total_out[...]
    norm = 0.5 / (blocks * 128 * n_dx * n_dy * n_dz)
    energy_out[0] = jnp.sum(jnp.where(lane1 < 64, total, 0.0)) * norm
    dhdl_out[0] = jnp.sum(jnp.where(lane1 < 64, 0.0, total)) * (-norm / lam)
    results = [
        pltpu.make_async_copy(energy_out, energy_hbm, out_sem.at[0]),
        pltpu.make_async_copy(dhdl_out, dhdl_hbm, out_sem.at[1]),
    ]
    for copy in results:
        copy.start()
    wait_bytes(leavers.at[pl.ds(0, len(leaves))], leave_send)
    wait_bytes(ghost.at[pl.ds(0, (len(halos) + 9) * blocks)], ici_send)

    @pl.when(leader)
    def _():
        wait_bytes(plane_sums.at[pl.ds(0, n_dy - 1)], plane_send)
        wait_bytes(line_sums.at[pl.ds(0, n_dx - 1)], line_send)
        wait_bytes(total_out, total_send)

    @pl.when(jnp.logical_not(leader))
    def _():
        wait_bytes(plane_sums.at[pl.ds(0, n_dy)], plane_send)

    for copy in results:
        copy.wait()


def on_device(
    fraction,
    atom_type,
    perturbed,
    leaving,
    neighbours,
    counts,
    sigma_table,
    depth_table,
    charge_table,
    domain_edge,
    coupling,
):
    n_dx, n_dy, n_dz = (lax.axis_size(axis) for axis in ("dx", "dy", "dz"))
    atoms = fraction.shape[-1]
    blocks = atoms // 128
    sizes = (n_dx, n_dy, n_dz, blocks, neighbours.shape[-1])
    neighbours = neighbours.transpose(0, 1, 3, 2, 4)
    hbm = pl.BlockSpec(memory_space=pltpu.HBM)
    dma, regular = pltpu.SemaphoreType.DMA, pltpu.SemaphoreType.REGULAR
    scalars = (
        leaving,
        neighbours,
        counts,
        sigma_table,
        depth_table,
        charge_table,
        domain_edge,
        coupling,
    )
    return pl.pallas_call(
        lambda *refs: kernel(sizes, *refs),
        out_shape=(
            pltpu.VMEM(fraction.shape, F32),
            jax.ShapeDtypeStruct((1,), F32),
            jax.ShapeDtypeStruct((1,), F32),
        ),
        in_specs=[hbm] * 11,
        out_specs=(pl.BlockSpec(memory_space=pltpu.VMEM), hbm, hbm),
        scratch_shapes=[
            pltpu.SMEM((1,), F32),
            pltpu.SMEM((1,), F32),
            *[pltpu.SMEM(array.shape, array.dtype) for array in scalars],
            pltpu.VMEM((2 * blocks, 128), jnp.int32),
            pltpu.VMEM((5 * blocks, 128), F32),
            pltpu.VMEM((4, blocks, 128), F32),
            pltpu.VMEM((9, blocks, 8, 128), F32),
            pltpu.VMEM((15, 2, 128), F32),
            pltpu.VMEM((15, 8, 128), F32),
            pltpu.VMEM((9, blocks, 16, 128), F32),
            pltpu.VMEM((9 * blocks, 8, 128), F32),
            pltpu.VMEM((27 * blocks + 1, 8, 128), F32),
            pltpu.SMEM((blocks * neighbours.shape[-1],), jnp.int32),
            pltpu.VMEM((atoms, 8), F32),
            pltpu.VMEM((8, atoms, 128), F32),
            pltpu.VMEM((3, atoms, 128), F32),
            pltpu.VMEM((n_dy * n_dz, 1, 128), F32),
            pltpu.VMEM((n_dx, 1, 128), F32),
            pltpu.VMEM((1, 128), F32),
            pltpu.VMEM((1, 128), F32),
            dma((len(scalars),)),
            *[dma] * 12,
            dma((2,)),
            regular((3,)),
        ],
        compiler_params=pltpu.CompilerParams(
            collective_id=0, has_side_effects=True, vmem_limit_bytes=62 * 1024 * 1024
        ),
        name="step",
    )(
        fraction,
        atom_type,
        perturbed,
        leaving,
        neighbours,
        counts,
        sigma_table,
        depth_table,
        charge_table,
        domain_edge,
        coupling,
    )


def solution(mesh):
    return jax.shard_map(
        on_device,
        mesh=mesh,
        in_specs=(
            P(None, ("win", "dx"), "dy", "dz", None),
            P(("win", "dx"), "dy", "dz", None),
            P(("win", "dx"), "dy", "dz", None),
            P(("win", "dx"), "dy", "dz", None, None),
            P(("win", "dx"), "dy", "dz", None, None),
            P(("win", "dx"), "dy", "dz", None),
            P(),
            P(),
            P(),
            P(),
            P("win"),
        ),
        out_specs=(P(None, ("win", "dx"), "dy", "dz", None), P("win"), P("win")),
        check_vma=False,
    )
```
